8 devices in a mesh: ep: 8 (over z, y, x, core).
Axes of the slice: x: 2, y: 2, z: 1, core: 2. Of those that a mesh axis runs over, the one named last changes fastest.
Arguments:
- tokens: bfloat16 [16, 2048, 2048], P('ep')
- loss_weight: bfloat16 [16, 2048, 2048], P('ep')
- w_gate: bfloat16 [2048, 64], replicated
- w_in: bfloat16 [64, 2048, 1024], P('ep')
- w_out: bfloat16 [64, 1024, 2048], P('ep')
- first_expert: int32 [16, 2048], P('ep')
- second_expert: int32 [16, 2048], P('ep')
- keep_second: int32 [16, 2048], P('ep')
Outputs:
- output 1: float32 [], replicated
- output 2: bfloat16 [16, 2048, 2048], P('ep')
- output 3: bfloat16 [64, 2048, 1024], P('ep')
- output 4: bfloat16 [64, 1024, 2048], P('ep')
- output 5: float32 [2048, 64], replicated
All inputs are finite; a program needn't handle non-finite values.
Results may differ from the reference program's by a relative error of at most 0.00956181.
Values are sent between devices in bfloat16 or wider.
A program may use at most 1 GiB of HBM per device.

```python
import jax
import jax.numpy as jnp
from jax import lax

EXPERTS = 64
HIDDEN = 2048
FF_DIM = 1024
SEQ_LEN = 2048
GROUPS = 16
CAPACITY = 2 * SEQ_LEN // EXPERTS
TOKENS = GROUPS * SEQ_LEN
NUMEL = TOKENS * HIDDEN
ALPHA = 0.01


def draw_routes(route_key):
    sub_keys = jax.random.split(route_key, 6)
    skew_level = jax.random.randint(sub_keys[0], (GROUPS, 1), 0, 4)
    hot_expert = jax.random.randint(sub_keys[1], (GROUPS, 1), 0, EXPERTS)
    hot_pick = jax.random.randint(sub_keys[2], (GROUPS, SEQ_LEN), 0, 8)
    spread = jax.random.randint(sub_keys[3], (GROUPS, SEQ_LEN), 0, EXPERTS)
    first_expert = jnp.where(hot_pick < skew_level, hot_expert, spread).astype(jnp.int32)
    offset = jax.random.randint(sub_keys[4], (GROUPS, SEQ_LEN), 1, EXPERTS)
    second_expert = ((first_expert + offset) % EXPERTS).astype(jnp.int32)
    keep_second = (jax.random.randint(sub_keys[5], (GROUPS, SEQ_LEN), 0, 3) > 0).astype(jnp.int32)
    return first_expert, second_expert, keep_second


def setup_inputs(seed: int = 0) -> dict:
    sub_keys = jax.random.split(jax.random.key(seed), 6)
    tokens = jax.random.normal(sub_keys[0], (GROUPS, SEQ_LEN, HIDDEN), jnp.float32).astype(jnp.bfloat16)
    loss_weight = jax.random.normal(sub_keys[1], (GROUPS, SEQ_LEN, HIDDEN), jnp.float32).astype(jnp.bfloat16)
    w_gate = (jax.random.normal(sub_keys[2], (HIDDEN, EXPERTS), jnp.float32) * HIDDEN ** -0.5).astype(jnp.bfloat16)
    w_in = (jax.random.normal(sub_keys[3], (EXPERTS, HIDDEN, FF_DIM), jnp.float32) * HIDDEN ** -0.5).astype(jnp.bfloat16)
    w_out = (jax.random.normal(sub_keys[4], (EXPERTS, FF_DIM, HIDDEN), jnp.float32) * FF_DIM ** -0.5).astype(jnp.bfloat16)
    first_expert, second_expert, keep_second = draw_routes(sub_keys[5])
    return {'tokens': tokens, 'loss_weight': loss_weight, 'w_gate': w_gate, 'w_in': w_in, 'w_out': w_out, 'first_expert': first_expert, 'second_expert': second_expert, 'keep_second': keep_second}


def table_for(hot_rows, pos_rows, kept_rows):
    slot_ids = jnp.arange(CAPACITY, dtype=jnp.int32)
    slot_hit = ((pos_rows[:, None, None] == slot_ids) & (kept_rows[:, None, None] > 0)).astype(jnp.float32)
    return hot_rows[:, :, None] * slot_hit


def expert_apply(packed):
    x_slots, w_first, w_second = packed
    pre_act = jnp.einsum('gch,hf->gcf', x_slots.astype(jnp.float32), w_first.astype(jnp.float32))
    act_bf = jax.nn.gelu(pre_act, approximate=True).astype(jnp.bfloat16)
    return jnp.einsum('gcf,fh->gch', act_bf.astype(jnp.float32), w_second.astype(jnp.float32)).astype(jnp.bfloat16)


def reference(tokens, loss_weight, w_gate, w_in, w_out, first_expert, second_expert, keep_second):
    expert_ids = jnp.arange(EXPERTS, dtype=jnp.int32)
    first_int = (first_expert[..., None] == expert_ids).astype(jnp.int32)
    second_int = (second_expert[..., None] == expert_ids).astype(jnp.int32)
    second_keep = second_int * keep_second[..., None]
    first_count = jnp.sum(first_int, axis=1)
    pos_first = jnp.sum((jnp.cumsum(first_int, axis=1) - first_int) * first_int, axis=-1)
    pos_second = jnp.sum((jnp.cumsum(second_keep, axis=1) - second_keep + first_count[:, None, :]) * second_int, axis=-1)
    kept_first = (pos_first < CAPACITY).astype(jnp.int32)
    kept_second = keep_second * (pos_second < CAPACITY).astype(jnp.int32)
    first_hot = first_int.astype(jnp.float32)
    second_hot = second_int.astype(jnp.float32)
    frac_first = jnp.sum(first_hot, axis=(0, 1)) / TOKENS

    def dispatch_group(packed):
        x_group, pos_one, kept_one, hot_one, pos_two, kept_two, hot_two = packed
        table = table_for(hot_one, pos_one, kept_one) + table_for(hot_two, pos_two, kept_two)
        return jnp.einsum('sec,sh->ech', table, x_group).astype(jnp.bfloat16)

    def combine_group(packed):
        y_group, pos_one, kept_one, hot_one, pos_two, kept_two, hot_two, norm_one, norm_two = packed
        combine = (table_for(hot_one, pos_one, kept_one) * norm_one[:, None, None] + table_for(hot_two, pos_two, kept_two) * norm_two[:, None, None]).astype(jnp.bfloat16)
        return jnp.einsum('sec,ech->sh', combine.astype(jnp.float32), y_group.astype(jnp.float32))

    def objective(x_in, gate_w, w_first, w_second):
        x_f32 = x_in.astype(jnp.float32)
        logits = jnp.einsum('gsh,he->gse', x_f32, gate_w)
        router_prob = jax.nn.softmax(logits, axis=-1)
        gate_first = jnp.sum(router_prob * first_hot, axis=-1)
        gate_second = jnp.sum(router_prob * second_hot, axis=-1)
        norm_first = gate_first / (gate_first + gate_second)
        norm_second = gate_second / (gate_first + gate_second)
        slots_in = lax.map(jax.checkpoint(dispatch_group), (x_f32, pos_first, kept_first, first_hot, pos_second, kept_second, second_hot))
        slots_out = lax.map(jax.checkpoint(expert_apply), (jnp.moveaxis(slots_in, 0, 1), w_first, w_second))
        moe_out = lax.map(jax.checkpoint(combine_group), (jnp.moveaxis(slots_out, 0, 1), pos_first, kept_first, first_hot, pos_second, kept_second, second_hot, norm_first, norm_second))
        dot_sum = jnp.sum((x_f32 + moe_out) * loss_weight.astype(jnp.float32))
        mean_prob = jnp.sum(router_prob, axis=(0, 1)) / TOKENS
        loss_value = dot_sum / NUMEL + ALPHA * EXPERTS * jnp.sum(frac_first * mean_prob)
        return loss_value * NUMEL, loss_value

    _, pull_back, loss_value = jax.vjp(objective, tokens, w_gate.astype(jnp.float32), w_in, w_out, has_aux=True)
    grad_x, grad_gate, grad_w_in, grad_w_out = pull_back(jnp.ones((), jnp.float32))
    return loss_value, grad_x, grad_w_in, grad_w_out, grad_gate
```

```python
import functools

import jax
import jax.numpy as jnp
from jax import lax
from jax.experimental import pallas as pl
from jax.experimental.pallas import tpu as pltpu
from jax.sharding import PartitionSpec as P


ALPHA = 0.01
LANES = 128
MIB = 1024 * 1024
BATCH = 16
bf16, f32 = jnp.bfloat16, jnp.float32


def gelu_bf16(pre_act):
    return jax.nn.gelu(pre_act, approximate=True).astype(bf16)


def cost(flops, moved):
    return pl.CostEstimate(flops=flops, bytes_accessed=moved, transcendentals=0)


def move_rows(idx_ref, base, count, load, store):
    def step(i, _):
        ids = [idx_ref[base + i * BATCH + u] for u in range(BATCH)]
        for u, row in enumerate([load(k) for k in ids]):
            store(i * BATCH + u, row)
        return 0

    lax.fori_loop(0, count // BATCH, step, 0)


def gather_kernel(idx_ref, tiles_ref, *outs, ranges, rows):
    base = pl.program_id(0) * rows
    for (low, high), out_ref in zip(ranges, outs):
        def store(t, row, out_ref=out_ref):
            out_ref[0, t] = row

        move_rows(idx_ref, base + low, high - low, lambda k: tiles_ref[k], store)


def gather_rows(idx, tiles, ranges):
    peers, rows = idx.shape
    count, sub, _ = tiles.shape
    return pl.pallas_call(
        functools.partial(gather_kernel, ranges=ranges, rows=rows),
        grid_spec=pltpu.PrefetchScalarGridSpec(
            num_scalar_prefetch=1,
            grid=(peers,),
            in_specs=[pl.BlockSpec((count, sub, LANES), lambda p, idx: (0, 0, 0))],
            out_specs=[pl.BlockSpec((1, high - low, sub, LANES), lambda p, idx: (p, 0, 0, 0)) for low, high in ranges],
        ),
        out_shape=[jax.ShapeDtypeStruct((peers, high - low, sub, LANES), tiles.dtype) for low, high in ranges],
        compiler_params=pltpu.CompilerParams(vmem_limit_bytes=52 * MIB),
        cost_estimate=cost(30_000_000_000, 60_000_000),
    )(idx.reshape(-1), tiles)


def unpack_kernel(idx_ref, *refs, ranges, scaled, empty, block):
    count = len(ranges)
    parts, refs = refs[:count], refs[count:]
    if scaled:
        norm_ref, y_ref, out_ref, dot_ref, packed, acc_ref, sem = refs
    else:
        out_ref, packed, acc_ref, sem = refs
    peer, local = pl.program_id(0), pl.program_id(1)
    slot = lax.rem(peer, 2)

    def copies(p, s):
        return [pltpu.make_async_copy(part.at[p], packed.at[s, pl.ds(low, high - low)], sem.at[s, k])
                for k, (part, (low, high)) in enumerate(zip(parts, ranges))]

    @pl.when((peer == 0) & (local == 0))
    def _():
        blank = jnp.zeros((2, packed.shape[1] - empty) + packed.shape[2:], bf16)
        packed[:, empty:] = blank
        for copy in copies(0, 0):
            copy.start()

    @pl.when(local == 0)
    def _():
        @pl.when(peer + 1 < pl.num_programs(0))
        def _():
            for copy in copies(peer + 1, 1 - slot):
                copy.start()

        for copy in copies(peer, slot):
            copy.wait()

    base = (peer * pl.num_programs(1) + local) * block
    sub = packed.shape[2]
    pitch = sub + 1

    def store(t, row):
        acc_ref[pl.ds(t * pitch, sub), :] = row.astype(f32)

    move_rows(idx_ref, base, block, lambda k: packed[slot, k], store)
    total = None
    for j in range(sub):
        cols = slice(j * LANES, (j + 1) * LANES)
        tile = acc_ref[pl.ds(j, block, stride=pitch), :]
        if scaled:
            out_ref[0, 0, :, cols] = (norm_ref[0, 0] * tile).astype(bf16)
            product = y_ref[0, 0, :, cols].astype(f32) * tile
            total = product if total is None else total + product
        else:
            out_ref[0, 0, :, cols] = tile.astype(bf16)
    if scaled:
        dot_ref[0, 0] = total


def unpack_rows(idx, parts, ranges, empty, norm=None, y=None, first=0):
    peers, local, block = idx.shape
    sub = parts[0].shape[2]
    hidden = sub * LANES
    scaled = norm is not None
    spec = lambda width, off=0: pl.BlockSpec((1, 1, block, width), lambda p, e, idx: (e + off, p, 0, 0))
    ins = [pl.BlockSpec(memory_space=pl.ANY)] * len(parts)
    out_shape = [jax.ShapeDtypeStruct((local, peers, block, hidden), bf16)]
    if scaled:
        ins += [spec(1, first), spec(hidden, first)]
        out_shape.append(jax.ShapeDtypeStruct((local, peers, block, LANES), f32))
    out = pl.pallas_call(
        functools.partial(unpack_kernel, ranges=ranges, scaled=scaled, empty=empty, block=block),
        grid_spec=pltpu.PrefetchScalarGridSpec(
            num_scalar_prefetch=1,
            grid=(peers, local),
            in_specs=ins,
            out_specs=[spec(s.shape[-1]) for s in out_shape],
            scratch_shapes=[
                pltpu.VMEM((2, empty + 8, sub, LANES), bf16),
                pltpu.VMEM((block * (sub + 1), LANES), f32),
                pltpu.SemaphoreType.DMA((2, len(parts))),
            ],
        ),
        out_shape=out_shape,
        compiler_params=pltpu.CompilerParams(vmem_limit_bytes=32 * MIB),
        cost_estimate=cost(3_500_000_000 * local, 8_000_000 * local),
    )(idx.reshape(-1), *parts, *((norm, y) if scaled else ()))
    return out if scaled else out[0]


def pack_kernel(idx_ref, *refs, ranges, rows, count):
    ins, outs, acc_ref = refs[:count], refs[count:-1], refs[-1]
    base = pl.program_id(0) * rows
    sub = outs[0].shape[2]
    pitch = sub + 1
    at = 0
    for ref in ins:
        for e in range(ref.shape[0]):
            block = ref.shape[2]
            for j in range(sub):
                acc_ref[pl.ds(at * pitch + j, block, stride=pitch), :] = ref[e, 0, :, j * LANES:(j + 1) * LANES].astype(f32)
            at += block
    for (low, high), out_ref in zip(ranges, outs):
        def store(t, row, out_ref=out_ref):
            out_ref[0, t] = row.astype(bf16)

        move_rows(idx_ref, base + low, high - low, lambda k: acc_ref[pl.ds(k * pitch, sub), :], store)


def pack_rows(idx, grads, ranges):
    peers, rows = idx.shape
    block, hidden = grads[0].shape[2:]
    sub = hidden // LANES
    total = sum(g.shape[0] for g in grads) * block
    return pl.pallas_call(
        functools.partial(pack_kernel, ranges=ranges, rows=rows, count=len(grads)),
        grid_spec=pltpu.PrefetchScalarGridSpec(
            num_scalar_prefetch=1,
            grid=(peers,),
            in_specs=[pl.BlockSpec((g.shape[0], 1, block, hidden), lambda p, idx: (0, p, 0, 0)) for g in grads],
            out_specs=[pl.BlockSpec((1, high - low, sub, LANES), lambda p, idx: (p, 0, 0, 0)) for low, high in ranges],
            scratch_shapes=[pltpu.VMEM((total * (sub + 1), LANES), f32)],
        ),
        out_shape=[jax.ShapeDtypeStruct((peers, high - low, sub, LANES), bf16) for low, high in ranges],
        compiler_params=pltpu.CompilerParams(vmem_limit_bytes=40 * MIB),
        cost_estimate=cost(15_000_000_000, 35_000_000),
    )(idx.reshape(-1), *grads)


def combine_kernel(slot_ref, *refs, ranges, rows):
    count = len(ranges)
    parts, (r_ref, gl_ref, wg_ref, out_ref, held, acc_ref, sem) = refs[:count], refs[count:]
    block = out_ref.shape[0]
    tokens = slot_ref.shape[0] // 2
    base = pl.program_id(0) * block

    sub = held.shape[1]
    pitch = sub + 1
    peers = parts[0].shape[0]

    @pl.when(pl.program_id(0) == 0)
    def _():
        copies = [pltpu.make_async_copy(part.at[p], held.at[pl.ds(p * rows + low, high - low)], sem.at[k, p])
                  for k, (part, (low, high)) in enumerate(zip(parts, ranges)) for p in range(peers)]
        for copy in copies:
            copy.start()
        held[peers * rows:] = jnp.zeros((held.shape[0] - peers * rows,) + held.shape[1:], bf16)
        for copy in copies:
            copy.wait()

    def step(i, _):
        ones = [slot_ref[base + i * 8 + u] for u in range(8)]
        twos = [slot_ref[base + tokens + i * 8 + u] for u in range(8)]
        sums = [held[one].astype(f32) + held[two].astype(f32) for one, two in zip(ones, twos)]
        for u, row in enumerate(sums):
            acc_ref[pl.ds((i * 8 + u) * pitch, sub), :] = row
        return 0

    lax.fori_loop(0, block // 8, step, 0)
    router = lax.dot_general(gl_ref[...], wg_ref[...], (((1,), (1,)), ((), ())), preferred_element_type=f32)
    for j in range(sub):
        cols = slice(j * LANES, (j + 1) * LANES)
        out_ref[:, cols] = (r_ref[:, cols].astype(f32) + acc_ref[pl.ds(j, block, stride=pitch), :] + router[:, cols]).astype(bf16)


def combine_rows(slots_of, parts, ranges, r_rows, grad_logits, w_gate):
    tokens, hidden = r_rows.shape
    experts = w_gate.shape[1]
    peers, sub = parts[0].shape[0], parts[0].shape[2]
    rows = ranges[-1][1]
    block = 256
    return pl.pallas_call(
        functools.partial(combine_kernel, ranges=ranges, rows=rows),
        grid_spec=pltpu.PrefetchScalarGridSpec(
            num_scalar_prefetch=1,
            grid=(tokens // block,),
            in_specs=[pl.BlockSpec(memory_space=pl.ANY)] * len(parts) + [
                pl.BlockSpec((block, hidden), lambda b, s: (b, 0)),
                pl.BlockSpec((block, experts), lambda b, s: (b, 0)),
                pl.BlockSpec((hidden, experts), lambda b, s: (0, 0)),
            ],
            out_specs=pl.BlockSpec((block, hidden), lambda b, s: (b, 0)),
            scratch_shapes=[
                pltpu.VMEM((peers * rows + 8, sub, LANES), bf16),
                pltpu.VMEM((block * (sub + 1), LANES), f32),
                pltpu.SemaphoreType.DMA((len(parts), peers)),
            ],
        ),
        out_shape=jax.ShapeDtypeStruct(r_rows.shape, bf16),
        compiler_params=pltpu.CompilerParams(vmem_limit_bytes=52 * MIB),
        cost_estimate=cost(50_000_000_000, 80_000_000),
    )(slots_of.reshape(-1), *parts, r_rows, grad_logits, w_gate)


def solution(mesh):
    ep_size = mesh.shape['ep']

    def layer_body(x_loc, r_loc, w_gate, w_in_loc, w_out_loc, first_ids, second_ids, keep_ids):
        groups, seq_len, hidden = x_loc.shape
        experts = w_gate.shape[1]
        local_experts = experts // ep_size
        half = local_experts // 2
        cap_rows = 2 * seq_len // experts
        block = groups * cap_rows
        rows = local_experts * block
        mid = rows // 2
        sub = hidden // LANES
        tokens_loc = groups * seq_len
        tokens_all = tokens_loc * ep_size
        numel = tokens_all * hidden
        me = lax.axis_index('ep')
        exchange = lambda v: lax.all_to_all(v, 'ep', 0, 0, tiled=True)

        expert_ids = jnp.arange(experts, dtype=jnp.int32)
        first_hot = (first_ids[..., None] == expert_ids).astype(bf16)
        second_hot = (second_ids[..., None] == expert_ids).astype(bf16)
        second_kept = second_hot * keep_ids.astype(bf16)[..., None]
        seq_ids = jnp.arange(seq_len, dtype=jnp.int32)
        earlier = (seq_ids[:, None] > seq_ids[None, :]).astype(bf16)
        before_first = jnp.einsum('st,gte->gse', earlier, first_hot, preferred_element_type=f32)
        before_second = jnp.einsum('st,gte->gse', earlier, second_kept, preferred_element_type=f32)
        first_count = jnp.sum(first_hot, axis=1, dtype=f32)
        occupied = jnp.minimum(first_count + jnp.sum(second_kept, axis=1, dtype=f32), cap_rows)
        segments = lambda v: jnp.moveaxis(v.reshape(groups, ep_size, local_experts), 0, 2).reshape(ep_size, local_experts * groups)
        held = segments(occupied)
        starts = jnp.cumsum(held, axis=1) - held
        lead = rows - jnp.sum(held, axis=1, keepdims=True)
        place = jnp.arange(ep_size, dtype=f32)[:, None] * rows + starts
        unsegment = lambda v: jnp.moveaxis(v.reshape(ep_size, local_experts, groups), 2, 0).reshape(groups, experts)
        place_of, lead_of = unsegment(place), unsegment(jnp.broadcast_to(lead, place.shape))

        def locate(hot, before):
            pos = jnp.sum(before * hot, axis=-1)
            there = jnp.sum(place_of[:, None, :] * hot, axis=-1) + pos
            back = there + jnp.sum(lead_of[:, None, :] * hot, axis=-1)
            return pos.astype(jnp.int32), there.astype(jnp.int32), back.astype(jnp.int32)

        pos_first, there_first, back_first = locate(first_hot, before_first)
        pos_second, there_second, back_second = locate(second_hot, before_second + first_count[:, None, :])
        ok_first = pos_first < cap_rows
        ok_second = (keep_ids > 0) & (pos_second < cap_rows)
        slots_of = jnp.stack([jnp.where(ok_first, back_first, ep_size * rows), jnp.where(ok_second, back_second, ep_size * rows)])

        there = jnp.stack([jnp.where(ok_first, there_first, -1), jnp.where(ok_second, there_second, -1)]).reshape(-1)
        numbers = jnp.arange(2 * tokens_loc, dtype=jnp.int32) % tokens_loc + 1
        outer = ((there // 64)[:, None] == jnp.arange(ep_size * rows // 64, dtype=jnp.int32)).astype(bf16)
        inner = ((there % 64)[:, None] == jnp.arange(64, dtype=jnp.int32)) & (there >= 0)[:, None]
        digits = jnp.concatenate([jnp.where(inner, v.astype(bf16)[:, None], 0) for v in (numbers // 64, numbers % 64)], axis=-1)
        table = jnp.einsum('so,si->oi', outer, digits, preferred_element_type=f32)
        send_idx = jnp.maximum((table[:, :64] * 64 + table[:, 64:]).astype(jnp.int32) - 1, 0).reshape(ep_size, rows)

        x_tiles = x_loc.reshape(tokens_loc, sub, LANES)
        r_tiles = r_loc.reshape(tokens_loc, sub, LANES)
        x_ranges = ((0, rows),)
        r_ranges = ((0, mid), (mid, rows))
        x_send, = gather_rows(send_idx, x_tiles, x_ranges)

        counts = lax.all_gather(jnp.stack([first_count, occupied]), 'ep')
        frac_first = jnp.sum(counts[:, 0], axis=(0, 1)) / tokens_all
        mine = lax.dynamic_slice_in_dim(counts[:, 1], me * local_experts, local_experts, axis=2)
        mine = jnp.moveaxis(mine, 1, 2).reshape(ep_size, local_experts * groups)
        mine_ends = jnp.cumsum(mine, axis=1)
        mine_starts = mine_ends - mine
        slot_ids = jnp.arange(cap_rows, dtype=f32)
        recv_idx = jnp.where(slot_ids < mine[..., None], mine_starts[..., None] + slot_ids, float(rows)).astype(jnp.int32)
        recv_idx = recv_idx.reshape(ep_size, local_experts, block)
        packed = jnp.arange(rows, dtype=f32) - (rows - mine_ends[:, -1:])
        passed = (mine_ends[:, None, :] <= packed[..., None]).astype(f32)
        back_row = jnp.sum(passed, axis=-1) * cap_rows + packed - jnp.sum(passed * mine[:, None, :], axis=-1)
        back_idx = jnp.where(packed >= 0, back_row, 0.0).astype(jnp.int32)

        tie = lambda *values: lax.optimization_barrier(values)
        x_send, recv_idx, back_idx, frac_first = tie(x_send, recv_idx, back_idx, frac_first)
        x_recv = exchange(x_send)
        x_here, r_here, r_tiles, _ = tie(x_loc, r_loc, r_tiles, x_send)
        r_send_0, r_send_1 = gather_rows(send_idx, r_tiles, r_ranges)

        logits = jnp.einsum('gsh,he->gse', x_here, w_gate, preferred_element_type=f32)
        router_prob = jax.nn.softmax(logits, axis=-1)
        gate_first = jnp.sum(router_prob * first_hot, axis=-1)
        gate_second = jnp.sum(router_prob * second_hot, axis=-1)
        gate_sum = gate_first + gate_second
        norm_first = (gate_first / gate_sum).astype(bf16)
        norm_second = (gate_second / gate_sum).astype(bf16)
        slots = jnp.arange(cap_rows, dtype=jnp.int32)
        at_first = ((pos_first[..., None] == slots) & ok_first[..., None]).astype(bf16)
        at_second = ((pos_second[..., None] == slots) & ok_second[..., None]).astype(bf16)
        hots = jnp.concatenate([first_hot, second_hot], axis=1)
        norm_at = jnp.concatenate([at_first * norm_first[..., None], at_second * norm_second[..., None]], axis=1)
        slot_norm = jnp.einsum('gse,gsk->egk', hots, norm_at, preferred_element_type=f32)
        dot_xr = jnp.sum(x_here.astype(f32) * r_here.astype(f32))
        slot_norm, x_recv = tie(slot_norm, x_recv)
        expert_norm = lax.all_to_all(slot_norm, 'ep', 0, 1, tiled=True).reshape(local_experts, ep_size, block)

        r_send_0, expert_norm, dot_xr = tie(r_send_0, expert_norm, dot_xr)
        r_recv_0 = exchange(r_send_0)
        expert_x = unpack_rows(recv_idx, [x_recv], x_ranges, rows).reshape(local_experts, -1, hidden)
        pre_act = jnp.einsum('ech,ehf->ecf', expert_x, w_in_loc, preferred_element_type=f32)
        act_bf = gelu_bf16(pre_act)
        expert_y = jnp.einsum('ecf,efh->ech', act_bf, w_out_loc, preferred_element_type=f32).astype(bf16)

        r_send_1, expert_y, r_recv_0 = tie(r_send_1, expert_y, r_recv_0)
        r_recv_1 = exchange(r_send_1)

        def expert_bwd(parts, ranges, which):
            chunk = slice(which * half, (which + 1) * half)
            grad_y, dots = unpack_rows(recv_idx[:, chunk], parts, ranges, rows, expert_norm[..., None], expert_y.reshape(local_experts, ep_size, block, hidden), which * half)
            slot_dot = jnp.sum(dots, axis=-1)
            grad_y = grad_y.reshape(half, -1, hidden)
            grad_act = jnp.einsum('ech,efh->ecf', grad_y, w_out_loc[chunk], preferred_element_type=f32).astype(bf16)
            grad_pre = jax.vjp(gelu_bf16, pre_act[chunk])[1](grad_act)[0].astype(bf16)
            grad_slots = jnp.einsum('ecf,ehf->ech', grad_pre, w_in_loc[chunk], preferred_element_type=f32).astype(bf16)
            return grad_y, grad_pre, slot_dot, grad_slots.reshape(half, ep_size, block, hidden)

        grad_y_0, grad_pre_0, slot_dot_0, grad_slots_0 = expert_bwd([r_recv_0], r_ranges[:1], 0)
        g_send_0, = pack_rows(back_idx, [grad_slots_0], ((0, mid),))
        g_send_0, r_recv_1 = tie(g_send_0, r_recv_1)
        g_recv_0 = exchange(g_send_0)
        grad_y_1, grad_pre_1, slot_dot_1, grad_slots_1 = expert_bwd([r_recv_0, r_recv_1], r_ranges, 1)
        g_send_1, = pack_rows(back_idx, [grad_slots_0, grad_slots_1], ((mid, rows),))
        slot_dot = jnp.concatenate([slot_dot_0, slot_dot_1], axis=0)
        slot_dot, g_send_1, g_recv_0 = tie(slot_dot, g_send_1, g_recv_0)
        home_dot = lax.all_to_all(slot_dot.reshape(local_experts, ep_size * groups, cap_rows), 'ep', 1, 0, tiled=True)
        g_send_1, home_dot = tie(g_send_1, home_dot)
        g_recv_1 = exchange(g_send_1)

        grad_y = jnp.concatenate([grad_y_0, grad_y_1], axis=0)
        grad_pre = jnp.concatenate([grad_pre_0, grad_pre_1], axis=0)
        grad_w_out = jnp.einsum('ecf,ech->efh', act_bf, grad_y, preferred_element_type=f32).astype(bf16)
        grad_w_in = jnp.einsum('ech,ecf->ehf', expert_x, grad_pre, preferred_element_type=f32).astype(bf16)

        picked = lambda hot, at: jnp.sum(jnp.einsum('gse,egk->gsk', hot.astype(f32), home_dot, precision=lax.Precision.HIGHEST, preferred_element_type=f32) * at, axis=-1)
        grad_norm_first = picked(first_hot, at_first).astype(bf16).astype(f32)
        grad_norm_second = picked(second_hot, at_second).astype(bf16).astype(f32)
        gate_sq = gate_sum * gate_sum
        grad_gate_first = (grad_norm_first - grad_norm_second) * gate_second / gate_sq
        grad_gate_second = (grad_norm_second - grad_norm_first) * gate_first / gate_sq
        grad_prob = grad_gate_first[..., None] * first_hot + grad_gate_second[..., None] * second_hot + (ALPHA * hidden * experts) * frac_first
        grad_logits = router_prob * (grad_prob - jnp.sum(router_prob * grad_prob, axis=-1, keepdims=True))
        grad_logits_bf = grad_logits.astype(bf16)
        grad_gate_w = jnp.einsum('gsh,gse->he', x_loc, grad_logits_bf, preferred_element_type=f32)
        dot_sum = dot_xr + jnp.sum(slot_dot * expert_norm)
        stats = jnp.stack([jnp.sum(router_prob, axis=(0, 1)), jnp.broadcast_to(dot_sum, (experts,))])
        summed = lax.psum(jnp.concatenate([grad_gate_w, stats], axis=0), 'ep')
        grad_gate_w, prob_sum, dot_sum = summed[:hidden], summed[hidden], summed[hidden + 1, 0]
        loss_value = dot_sum / numel + ALPHA * experts * jnp.sum(frac_first * prob_sum / tokens_all)

        grad_x = combine_rows(slots_of, [g_recv_0, g_recv_1], ((0, mid), (mid, rows)), r_loc.reshape(-1, hidden), grad_logits_bf.reshape(-1, experts), w_gate)
        return loss_value, grad_x.reshape(x_loc.shape), grad_w_in, grad_w_out, grad_gate_w

    row_spec = P('ep', None, None)
    id_spec = P('ep', None)
    return jax.shard_map(layer_body, mesh=mesh, in_specs=(row_spec, row_spec, P(None, None), row_spec, row_spec, id_spec, id_spec, id_spec), out_specs=(P(), row_spec, row_spec, row_spec, P(None, None)), check_vma=False)
```

```python
import functools

import jax
import jax.numpy as jnp
from jax import lax
from jax.experimental import pallas as pl
from jax.experimental.pallas import tpu as pltpu
from jax.sharding import PartitionSpec as P


ALPHA = 0.01
LANES = 128
MIB = 1024 * 1024
BATCH = 16
BASE = 27
MORE = 32
bf16, f32 = jnp.bfloat16, jnp.float32


def gelu_bf16(pre_act):
    return jax.nn.gelu(pre_act, approximate=True).astype(bf16)


def cost(flops, moved):
    return pl.CostEstimate(flops=flops, bytes_accessed=moved, transcendentals=0)


def move_rows(idx_ref, base, count, load, store):
    def step(i, _):
        ids = [idx_ref[base + i * BATCH + u] for u in range(BATCH)]
        for u, row in enumerate([load(k) for k in ids]):
            store(i * BATCH + u, row)
        return 0

    lax.fori_loop(0, count // BATCH, step, 0)


def gather_kernel(idx_ref, tiles_ref, *outs, ranges, rows):
    base = pl.program_id(0) * rows
    for (low, high), out_ref in zip(ranges, outs):
        def store(t, row, out_ref=out_ref):
            out_ref[0, t] = row

        move_rows(idx_ref, base + low, high - low, lambda k: tiles_ref[k], store)


def gather_rows(idx, tiles, ranges):
    peers, rows = idx.shape
    count, sub, _ = tiles.shape
    return pl.pallas_call(
        functools.partial(gather_kernel, ranges=ranges, rows=rows),
        grid_spec=pltpu.PrefetchScalarGridSpec(
            num_scalar_prefetch=1,
            grid=(peers,),
            in_specs=[pl.BlockSpec((count, sub, LANES), lambda p, idx: (0, 0, 0))],
            out_specs=[pl.BlockSpec((1, high - low, sub, LANES), lambda p, idx: (p, 0, 0, 0)) for low, high in ranges],
        ),
        out_shape=[jax.ShapeDtypeStruct((peers, high - low, sub, LANES), tiles.dtype) for low, high in ranges],
        compiler_params=pltpu.CompilerParams(vmem_limit_bytes=52 * MIB),
        cost_estimate=cost(30_000_000_000, 60_000_000),
    )(idx.reshape(-1), tiles)


def unpack_kernel(idx_ref, *refs, ranges, scaled, empty, block):
    count = len(ranges)
    parts, refs = refs[:count], refs[count:]
    if scaled:
        norm_ref, y_ref, out_ref, dot_ref, packed, acc_ref, sem = refs
    else:
        out_ref, packed, acc_ref, sem = refs
    peer, local = pl.program_id(0), pl.program_id(1)
    slot = lax.rem(peer, 2)

    def copies(p, s):
        return [pltpu.make_async_copy(part.at[p, pl.ds(at, high - low)], packed.at[s, pl.ds(low, high - low)], sem.at[s, k])
                for k, (part, (low, high, at)) in enumerate(zip(parts, ranges))]

    @pl.when((peer == 0) & (local == 0))
    def _():
        blank = jnp.zeros((2, packed.shape[1] - empty) + packed.shape[2:], bf16)
        packed[:, empty:] = blank
        for copy in copies(0, 0):
            copy.start()

    @pl.when(local == 0)
    def _():
        @pl.when(peer + 1 < pl.num_programs(0))
        def _():
            for copy in copies(peer + 1, 1 - slot):
                copy.start()

        for copy in copies(peer, slot):
            copy.wait()

    base = (peer * pl.num_programs(1) + local) * block
    sub = packed.shape[2]
    pitch = sub + 1

    def store(t, row):
        acc_ref[pl.ds(t * pitch, sub), :] = row.astype(f32)

    move_rows(idx_ref, base, block, lambda k: packed[slot, k], store)
    total = None
    for j in range(sub):
        cols = slice(j * LANES, (j + 1) * LANES)
        tile = acc_ref[pl.ds(j, block, stride=pitch), :]
        if scaled:
            out_ref[0, 0, :, cols] = (norm_ref[0, 0] * tile).astype(bf16)
            product = y_ref[0, 0, :, cols].astype(f32) * tile
            total = product if total is None else total + product
        else:
            out_ref[0, 0, :, cols] = tile.astype(bf16)
    if scaled:
        dot_ref[0, 0] = total


def unpack_rows(idx, parts, ranges, empty, norm=None, y=None, first=0):
    peers, local, block = idx.shape
    sub = parts[0].shape[2]
    hidden = sub * LANES
    scaled = norm is not None
    spec = lambda width, off=0: pl.BlockSpec((1, 1, block, width), lambda p, e, idx: (e + off, p, 0, 0))
    ins = [pl.BlockSpec(memory_space=pl.ANY)] * len(parts)
    out_shape = [jax.ShapeDtypeStruct((local, peers, block, hidden), bf16)]
    if scaled:
        ins += [spec(1, first), spec(hidden, first)]
        out_shape.append(jax.ShapeDtypeStruct((local, peers, block, LANES), f32))
    out = pl.pallas_call(
        functools.partial(unpack_kernel, ranges=ranges, scaled=scaled, empty=empty, block=block),
        grid_spec=pltpu.PrefetchScalarGridSpec(
            num_scalar_prefetch=1,
            grid=(peers, local),
            in_specs=ins,
            out_specs=[spec(s.shape[-1]) for s in out_shape],
            scratch_shapes=[
                pltpu.VMEM((2, empty + 8, sub, LANES), bf16),
                pltpu.VMEM((block * (sub + 1), LANES), f32),
                pltpu.SemaphoreType.DMA((2, len(parts))),
            ],
        ),
        out_shape=out_shape,
        compiler_params=pltpu.CompilerParams(vmem_limit_bytes=32 * MIB),
        cost_estimate=cost(3_500_000_000 * local, 8_000_000 * local),
    )(idx.reshape(-1), *parts, *((norm, y) if scaled else ()))
    return out if scaled else out[0]


def pack_kernel(idx_ref, *refs, ranges, rows, count):
    ins, outs, acc_ref = refs[:count], refs[count:-1], refs[-1]
    base = pl.program_id(0) * rows
    sub = outs[0].shape[2]
    pitch = sub + 1
    at = 0
    for ref in ins:
        for e in range(ref.shape[0]):
            block = ref.shape[2]
            for j in range(sub):
                acc_ref[pl.ds(at * pitch + j, block, stride=pitch), :] = ref[e, 0, :, j * LANES:(j + 1) * LANES].astype(f32)
            at += block
    for (low, high), out_ref in zip(ranges, outs):
        def store(t, row, out_ref=out_ref):
            out_ref[0, t] = row.astype(bf16)

        move_rows(idx_ref, base + low, high - low, lambda k: acc_ref[pl.ds(k * pitch, sub), :], store)


def pack_rows(idx, grads, ranges):
    peers, rows = idx.shape
    block, hidden = grads[0].shape[2:]
    sub = hidden // LANES
    total = sum(g.shape[0] for g in grads) * block
    return pl.pallas_call(
        functools.partial(pack_kernel, ranges=ranges, rows=rows, count=len(grads)),
        grid_spec=pltpu.PrefetchScalarGridSpec(
            num_scalar_prefetch=1,
            grid=(peers,),
            in_specs=[pl.BlockSpec((g.shape[0], 1, block, hidden), lambda p, idx: (0, p, 0, 0)) for g in grads],
            out_specs=[pl.BlockSpec((1, high - low, sub, LANES), lambda p, idx: (p, 0, 0, 0)) for low, high in ranges],
            scratch_shapes=[pltpu.VMEM((total * (sub + 1), LANES), f32)],
        ),
        out_shape=[jax.ShapeDtypeStruct((peers, high - low, sub, LANES), bf16) for low, high in ranges],
        compiler_params=pltpu.CompilerParams(vmem_limit_bytes=40 * MIB),
        cost_estimate=cost(15_000_000_000, 35_000_000),
    )(idx.reshape(-1), *grads)


def combine_kernel(slot_ref, *refs, ranges, rows):
    count = len(ranges)
    parts, (r_ref, gl_ref, wg_ref, out_ref, held, acc_ref, sem) = refs[:count], refs[count:]
    block = out_ref.shape[0]
    tokens = slot_ref.shape[0] // 2
    base = pl.program_id(0) * block

    sub = held.shape[1]
    pitch = sub + 1
    peers = parts[0].shape[0]

    @pl.when(pl.program_id(0) == 0)
    def _():
        copies = [pltpu.make_async_copy(part.at[p], held.at[pl.ds(p * rows + low, high - low)], sem.at[k, p])
                  for k, (part, (low, high)) in enumerate(zip(parts, ranges)) for p in range(peers)]
        for copy in copies:
            copy.start()
        held[peers * rows:] = jnp.zeros((held.shape[0] - peers * rows,) + held.shape[1:], bf16)
        for copy in copies:
            copy.wait()

    def step(i, _):
        ones = [slot_ref[base + i * 8 + u] for u in range(8)]
        twos = [slot_ref[base + tokens + i * 8 + u] for u in range(8)]
        sums = [held[one].astype(f32) + held[two].astype(f32) for one, two in zip(ones, twos)]
        for u, row in enumerate(sums):
            acc_ref[pl.ds((i * 8 + u) * pitch, sub), :] = row
        return 0

    lax.fori_loop(0, block // 8, step, 0)
    router = lax.dot_general(gl_ref[...], wg_ref[...], (((1,), (1,)), ((), ())), preferred_element_type=f32)
    for j in range(sub):
        cols = slice(j * LANES, (j + 1) * LANES)
        out_ref[:, cols] = (r_ref[:, cols].astype(f32) + acc_ref[pl.ds(j, block, stride=pitch), :] + router[:, cols]).astype(bf16)


def combine_rows(slots_of, parts, ranges, r_rows, grad_logits, w_gate):
    tokens, hidden = r_rows.shape
    experts = w_gate.shape[1]
    peers, sub = parts[0].shape[0], parts[0].shape[2]
    rows = ranges[-1][1]
    block = 256
    return pl.pallas_call(
        functools.partial(combine_kernel, ranges=ranges, rows=rows),
        grid_spec=pltpu.PrefetchScalarGridSpec(
            num_scalar_prefetch=1,
            grid=(tokens // block,),
            in_specs=[pl.BlockSpec(memory_space=pl.ANY)] * len(parts) + [
                pl.BlockSpec((block, hidden), lambda b, s: (b, 0)),
                pl.BlockSpec((block, experts), lambda b, s: (b, 0)),
                pl.BlockSpec((hidden, experts), lambda b, s: (0, 0)),
            ],
            out_specs=pl.BlockSpec((block, hidden), lambda b, s: (b, 0)),
            scratch_shapes=[
                pltpu.VMEM((peers * rows + 8, sub, LANES), bf16),
                pltpu.VMEM((block * (sub + 1), LANES), f32),
                pltpu.SemaphoreType.DMA((len(parts), peers)),
            ],
        ),
        out_shape=jax.ShapeDtypeStruct(r_rows.shape, bf16),
        compiler_params=pltpu.CompilerParams(vmem_limit_bytes=52 * MIB),
        cost_estimate=cost(50_000_000_000, 80_000_000),
    )(slots_of.reshape(-1), *parts, r_rows, grad_logits, w_gate)


def solution(mesh):
    ep_size = mesh.shape['ep']

    def layer_body(x_loc, r_loc, w_gate, w_in_loc, w_out_loc, first_ids, second_ids, keep_ids):
        groups, seq_len, hidden = x_loc.shape
        experts = w_gate.shape[1]
        local_experts = experts // ep_size
        half = local_experts // 2
        cap_rows = 2 * seq_len // experts
        block = groups * cap_rows
        rows = local_experts * block
        mid = rows // 2
        base = rows * BASE // 32
        over = rows - base
        sub = hidden // LANES
        tokens_loc = groups * seq_len
        tokens_all = tokens_loc * ep_size
        numel = tokens_all * hidden
        exchange = lambda v: lax.all_to_all(v, 'ep', 0, 0, tiled=True)

        expert_ids = jnp.arange(experts, dtype=jnp.int32)
        first_hot = (first_ids[..., None] == expert_ids).astype(bf16)
        second_hot = (second_ids[..., None] == expert_ids).astype(bf16)
        second_kept = second_hot * keep_ids.astype(bf16)[..., None]
        seq_ids = jnp.arange(seq_len, dtype=jnp.int32)
        earlier = (seq_ids[:, None] > seq_ids[None, :]).astype(bf16)
        before_first = jnp.einsum('st,gte->gse', earlier, first_hot, preferred_element_type=f32)
        before_second = jnp.einsum('st,gte->gse', earlier, second_kept, preferred_element_type=f32)
        first_count = jnp.sum(first_hot, axis=1, dtype=f32)
        occupied = jnp.minimum(first_count + jnp.sum(second_kept, axis=1, dtype=f32), cap_rows)
        segments = lambda v: jnp.moveaxis(v.reshape(groups, ep_size, local_experts), 0, 2).reshape(ep_size, local_experts * groups)
        held = segments(occupied)
        starts = jnp.cumsum(held, axis=1) - held
        lead = rows - jnp.sum(held, axis=1, keepdims=True)
        place = jnp.arange(ep_size, dtype=f32)[:, None] * rows + starts
        unsegment = lambda v: jnp.moveaxis(v.reshape(ep_size, local_experts, groups), 2, 0).reshape(groups, experts)
        place_of, lead_of = unsegment(place), unsegment(jnp.broadcast_to(lead, place.shape))

        def locate(hot, before):
            pos = jnp.sum(before * hot, axis=-1)
            there = jnp.sum(place_of[:, None, :] * hot, axis=-1) + pos
            back = there + jnp.sum(lead_of[:, None, :] * hot, axis=-1)
            return pos.astype(jnp.int32), there.astype(jnp.int32), back.astype(jnp.int32)

        pos_first, there_first, back_first = locate(first_hot, before_first)
        pos_second, there_second, back_second = locate(second_hot, before_second + first_count[:, None, :])
        ok_first = pos_first < cap_rows
        ok_second = (keep_ids > 0) & (pos_second < cap_rows)
        slots_of = jnp.stack([jnp.where(ok_first, back_first, ep_size * rows), jnp.where(ok_second, back_second, ep_size * rows)])

        there = jnp.stack([jnp.where(ok_first, there_first, -1), jnp.where(ok_second, there_second, -1)]).reshape(-1)
        numbers = jnp.arange(2 * tokens_loc, dtype=jnp.int32) % tokens_loc + 1
        outer = ((there // 64)[:, None] == jnp.arange(ep_size * rows // 64, dtype=jnp.int32)).astype(bf16)
        inner = ((there % 64)[:, None] == jnp.arange(64, dtype=jnp.int32)) & (there >= 0)[:, None]
        digits = jnp.concatenate([jnp.where(inner, v.astype(bf16)[:, None], 0) for v in (numbers // 64, numbers % 64)], axis=-1)
        table = jnp.einsum('so,si->oi', outer, digits, preferred_element_type=f32)
        send_idx = jnp.maximum((table[:, :64] * 64 + table[:, 64:]).astype(jnp.int32) - 1, 0).reshape(ep_size, rows)

        x_tiles = x_loc.reshape(tokens_loc, sub, LANES)
        r_tiles = r_loc.reshape(tokens_loc, sub, LANES)
        more = base + MORE
        x_ranges = ((0, base), (base, more), (more, rows))
        r_ranges = ((0, mid), (mid, base), (base, more), (more, rows))
        g_ranges = ((0, over - MORE), (over - MORE, over), (over, mid), (mid, rows))
        x_from = ((0, base, 0), (base, more, 0), (more, rows, 0))
        r_from = ((0, mid, 0), (mid, base, 0), (base, more, MORE), (more, rows, over - MORE))
        x_send, x_more, x_rest = gather_rows(send_idx, x_tiles, x_ranges)

        tie = lambda *values: lax.optimization_barrier(values)
        x_recv = exchange(x_send)
        x_here, r_here, r_tiles, _ = tie(x_loc, r_loc, r_tiles, x_send)
        r_send_0, r_send_1, r_more, r_rest = gather_rows(send_idx, r_tiles, r_ranges)

        logits = jnp.einsum('gsh,he->gse', x_here, w_gate, preferred_element_type=f32)
        router_prob = jax.nn.softmax(logits, axis=-1)
        gate_first = jnp.sum(router_prob * first_hot, axis=-1)
        gate_second = jnp.sum(router_prob * second_hot, axis=-1)
        gate_sum = gate_first + gate_second
        norm_first = (gate_first / gate_sum).astype(bf16)
        norm_second = (gate_second / gate_sum).astype(bf16)
        slots = jnp.arange(cap_rows, dtype=jnp.int32)
        at_first = ((pos_first[..., None] == slots) & ok_first[..., None]).astype(bf16)
        at_second = ((pos_second[..., None] == slots) & ok_second[..., None]).astype(bf16)
        hots = jnp.concatenate([first_hot, second_hot], axis=1)
        norm_at = jnp.concatenate([at_first * norm_first[..., None], at_second * norm_second[..., None]], axis=1)
        slot_norm = jnp.einsum('gse,gsk->egk', hots, norm_at, preferred_element_type=f32)
        dot_xr = jnp.sum(x_here.astype(f32) * r_here.astype(f32))
        to_rows = lambda v: jnp.moveaxis(v, 0, 1)[..., None]
        fullest = jnp.broadcast_to(jnp.max(jnp.sum(held, axis=1)), (experts, groups, 1))
        tally = jnp.moveaxis(first_count.reshape(groups, local_experts, ep_size), 0, 1)
        tally = jnp.tile(tally, (ep_size, 1, 1))
        sheet = jnp.concatenate([slot_norm, to_rows(occupied), fullest, tally], axis=-1)
        sheet, x_recv = tie(sheet, x_recv)
        sheet = lax.all_to_all(sheet, 'ep', 0, 1, tiled=True).reshape(local_experts, ep_size, groups, -1)
        expert_norm = sheet[..., :cap_rows].reshape(local_experts, ep_size, block)
        mine = jnp.moveaxis(sheet[..., cap_rows], 0, 1).reshape(ep_size, local_experts * groups)
        excess = jnp.max(sheet[0, :, 0, cap_rows + 1]) - base
        level = jnp.where(excess <= 0, 0, jnp.where(excess <= MORE, 1, 2)).astype(jnp.int32)
        frac_first = jnp.sum(sheet[..., cap_rows + 2:], axis=(1, 2)).reshape(experts) / tokens_all
        mine_ends = jnp.cumsum(mine, axis=1)
        mine_starts = mine_ends - mine
        slot_ids = jnp.arange(cap_rows, dtype=f32)
        recv_idx = jnp.where(slot_ids < mine[..., None], mine_starts[..., None] + slot_ids, float(rows)).astype(jnp.int32)
        recv_idx = recv_idx.reshape(ep_size, local_experts, block)
        packed = jnp.arange(rows, dtype=f32) - (rows - mine_ends[:, -1:])
        passed = (mine_ends[:, None, :] <= packed[..., None]).astype(f32)
        back_row = jnp.sum(passed, axis=-1) * cap_rows + packed - jnp.sum(passed * mine[:, None, :], axis=-1)
        back_idx = jnp.where(packed >= 0, back_row, 0.0).astype(jnp.int32)

        def exchange_over(few, rest):
            return lax.switch(level, (lambda u, v: (u, v), lambda u, v: (exchange(u), v), lambda u, v: (exchange(u), exchange(v))), few, rest)

        xr_more, xr_rest = jnp.concatenate([x_more, r_more], axis=1), jnp.concatenate([x_rest, r_rest], axis=1)
        xr_more, xr_rest, expert_norm = tie(xr_more, xr_rest, expert_norm)
        xr_more, xr_rest = exchange_over(xr_more, xr_rest)
        r_send_0, xr_more, xr_rest, dot_xr = tie(r_send_0, xr_more, xr_rest, dot_xr)
        r_recv_0 = exchange(r_send_0)
        expert_x = unpack_rows(recv_idx, [x_recv, xr_more, xr_rest], x_from, rows).reshape(local_experts, -1, hidden)
        pre_act = jnp.einsum('ech,ehf->ecf', expert_x, w_in_loc, preferred_element_type=f32)
        act_bf = gelu_bf16(pre_act)
        expert_y = jnp.einsum('ecf,efh->ech', act_bf, w_out_loc, preferred_element_type=f32).astype(bf16)

        r_send_1, expert_y, r_recv_0 = tie(r_send_1, expert_y, r_recv_0)
        r_recv_1 = exchange(r_send_1)

        def expert_bwd(parts, ranges, which):
            chunk = slice(which * half, (which + 1) * half)
            grad_y, dots = unpack_rows(recv_idx[:, chunk], parts, ranges, rows, expert_norm[..., None], expert_y.reshape(local_experts, ep_size, block, hidden), which * half)
            slot_dot = jnp.sum(dots, axis=-1)
            grad_y = grad_y.reshape(half, -1, hidden)
            grad_act = jnp.einsum('ech,efh->ecf', grad_y, w_out_loc[chunk], preferred_element_type=f32).astype(bf16)
            grad_pre = jax.vjp(gelu_bf16, pre_act[chunk])[1](grad_act)[0].astype(bf16)
            grad_slots = jnp.einsum('ecf,ehf->ech', grad_pre, w_in_loc[chunk], preferred_element_type=f32).astype(bf16)
            return grad_y, grad_pre, slot_dot, grad_slots.reshape(half, ep_size, block, hidden)

        grad_y_0, grad_pre_0, slot_dot_0, grad_slots_0 = expert_bwd([r_recv_0], r_from[:1], 0)
        g_rest, g_more, g_send_0 = pack_rows(back_idx, [grad_slots_0], g_ranges[:3])
        g_more, g_rest, r_recv_1 = tie(g_more, g_rest, r_recv_1)
        g_more, g_rest = exchange_over(g_more, g_rest)
        g_send_0, g_more, g_rest, r_recv_1 = tie(g_send_0, g_more, g_rest, r_recv_1)
        g_recv_0 = exchange(g_send_0)
        grad_y_1, grad_pre_1, slot_dot_1, grad_slots_1 = expert_bwd([r_recv_0, r_recv_1, xr_more, xr_rest], r_from, 1)
        g_send_1, = pack_rows(back_idx, [grad_slots_0, grad_slots_1], g_ranges[3:])
        slot_dot = jnp.concatenate([slot_dot_0, slot_dot_1], axis=0)
        slot_dot, g_send_1, g_recv_0 = tie(slot_dot, g_send_1, g_recv_0)
        home_dot = lax.all_to_all(slot_dot.reshape(local_experts, ep_size * groups, cap_rows), 'ep', 1, 0, tiled=True)
        g_send_1, home_dot = tie(g_send_1, home_dot)
        g_recv_1 = exchange(g_send_1)

        grad_y = jnp.concatenate([grad_y_0, grad_y_1], axis=0)
        grad_pre = jnp.concatenate([grad_pre_0, grad_pre_1], axis=0)
        grad_w_out = jnp.einsum('ecf,ech->efh', act_bf, grad_y, preferred_element_type=f32).astype(bf16)
        grad_w_in = jnp.einsum('ech,ecf->ehf', expert_x, grad_pre, preferred_element_type=f32).astype(bf16)

        picked = lambda hot, at: jnp.sum(jnp.einsum('gse,egk->gsk', hot.astype(f32), home_dot, precision=lax.Precision.HIGHEST, preferred_element_type=f32) * at, axis=-1)
        grad_norm_first = picked(first_hot, at_first).astype(bf16).astype(f32)
        grad_norm_second = picked(second_hot, at_second).astype(bf16).astype(f32)
        gate_sq = gate_sum * gate_sum
        grad_gate_first = (grad_norm_first - grad_norm_second) * gate_second / gate_sq
        grad_gate_second = (grad_norm_second - grad_norm_first) * gate_first / gate_sq
        grad_prob = grad_gate_first[..., None] * first_hot + grad_gate_second[..., None] * second_hot + (ALPHA * hidden * experts) * frac_first
        grad_logits = router_prob * (grad_prob - jnp.sum(router_prob * grad_prob, axis=-1, keepdims=True))
        grad_logits_bf = grad_logits.astype(bf16)
        grad_gate_w = jnp.einsum('gsh,gse->he', x_loc, grad_logits_bf, preferred_element_type=f32)
        dot_sum = dot_xr + jnp.sum(slot_dot * expert_norm)
        stats = jnp.stack([jnp.sum(router_prob, axis=(0, 1)), jnp.broadcast_to(dot_sum, (experts,))])
        summed = lax.psum(jnp.concatenate([grad_gate_w, stats], axis=0), 'ep')
        grad_gate_w, prob_sum, dot_sum = summed[:hidden], summed[hidden], summed[hidden + 1, 0]
        loss_value = dot_sum / numel + ALPHA * experts * jnp.sum(frac_first * prob_sum / tokens_all)

        grad_x = combine_rows(slots_of, [g_rest, g_more, g_recv_0, g_recv_1], g_ranges, r_loc.reshape(-1, hidden), grad_logits_bf.reshape(-1, experts), w_gate)
        return loss_value, grad_x.reshape(x_loc.shape), grad_w_in, grad_w_out, grad_gate_w

    row_spec = P('ep', None, None)
    id_spec = P('ep', None)
    return jax.shard_map(layer_body, mesh=mesh, in_specs=(row_spec, row_spec, P(None, None), row_spec, row_spec, id_spec, id_spec, id_spec), out_specs=(P(), row_spec, row_spec, row_spec, P(None, None)), check_vma=False)
```

```python
import functools

import jax
import jax.numpy as jnp
from jax import lax
from jax.experimental import pallas as pl
from jax.experimental.pallas import tpu as pltpu
from jax.sharding import PartitionSpec as P


ALPHA = 0.01
LANES = 128
MIB = 1024 * 1024
BATCH = 16
BASE_OUT, BASE_BACK = 26, 27
MORE = 32
bf16, f32 = jnp.bfloat16, jnp.float32


def gelu_bf16(pre_act):
    return jax.nn.gelu(pre_act, approximate=True).astype(bf16)


def cost(flops, moved):
    return pl.CostEstimate(flops=flops, bytes_accessed=moved, transcendentals=0)


def move_rows(idx_ref, base, count, load, store):
    def step(i, _):
        ids = [idx_ref[base + i * BATCH + u] for u in range(BATCH)]
        for u, row in enumerate([load(k) for k in ids]):
            store(i * BATCH + u, row)
        return 0

    lax.fori_loop(0, count // BATCH, step, 0)


def gather_kernel(idx_ref, tiles_ref, *outs, ranges, rows):
    base = pl.program_id(0) * rows
    for (low, high), out_ref in zip(ranges, outs):
        def store(t, row, out_ref=out_ref):
            out_ref[0, t] = row

        move_rows(idx_ref, base + low, high - low, lambda k: tiles_ref[k], store)


def gather_rows(idx, tiles, ranges):
    peers, rows = idx.shape
    count, sub, _ = tiles.shape
    return pl.pallas_call(
        functools.partial(gather_kernel, ranges=ranges, rows=rows),
        grid_spec=pltpu.PrefetchScalarGridSpec(
            num_scalar_prefetch=1,
            grid=(peers,),
            in_specs=[pl.BlockSpec((count, sub, LANES), lambda p, idx: (0, 0, 0))],
            out_specs=[pl.BlockSpec((1, high - low, sub, LANES), lambda p, idx: (p, 0, 0, 0)) for low, high in ranges],
        ),
        out_shape=[jax.ShapeDtypeStruct((peers, high - low, sub, LANES), tiles.dtype) for low, high in ranges],
        compiler_params=pltpu.CompilerParams(vmem_limit_bytes=52 * MIB),
        cost_estimate=cost(30_000_000_000, 60_000_000),
    )(idx.reshape(-1), tiles)


def unpack_kernel(idx_ref, *refs, ranges, scaled, empty, block):
    count = len(ranges)
    parts, refs = refs[:count], refs[count:]
    if scaled:
        norm_ref, y_ref, out_ref, dot_ref, packed, acc_ref, sem = refs
    else:
        out_ref, packed, acc_ref, sem = refs
    peer, local = pl.program_id(0), pl.program_id(1)
    slot = lax.rem(peer, 2)

    def copies(p, s):
        return [pltpu.make_async_copy(part.at[p, pl.ds(at, high - low)], packed.at[s, pl.ds(low, high - low)], sem.at[s, k])
                for k, (part, (low, high, at)) in enumerate(zip(parts, ranges))]

    @pl.when((peer == 0) & (local == 0))
    def _():
        blank = jnp.zeros((2, packed.shape[1] - empty) + packed.shape[2:], bf16)
        packed[:, empty:] = blank
        for copy in copies(0, 0):
            copy.start()

    @pl.when(local == 0)
    def _():
        @pl.when(peer + 1 < pl.num_programs(0))
        def _():
            for copy in copies(peer + 1, 1 - slot):
                copy.start()

        for copy in copies(peer, slot):
            copy.wait()

    base = (peer * pl.num_programs(1) + local) * block
    sub = packed.shape[2]
    pitch = sub + 1

    def store(t, row):
        acc_ref[pl.ds(t * pitch, sub), :] = row.astype(f32)

    move_rows(idx_ref, base, block, lambda k: packed[slot, k], store)
    total = None
    for j in range(sub):
        cols = slice(j * LANES, (j + 1) * LANES)
        tile = acc_ref[pl.ds(j, block, stride=pitch), :]
        if scaled:
            out_ref[0, 0, :, cols] = (norm_ref[0, 0] * tile).astype(bf16)
            product = y_ref[0, 0, :, cols].astype(f32) * tile
            total = product if total is None else total + product
        else:
            out_ref[0, 0, :, cols] = tile.astype(bf16)
    if scaled:
        dot_ref[0, 0] = total


def unpack_rows(idx, parts, ranges, empty, norm=None, y=None, first=0):
    peers, local, block = idx.shape
    sub = parts[0].shape[2]
    hidden = sub * LANES
    scaled = norm is not None
    spec = lambda width, off=0: pl.BlockSpec((1, 1, block, width), lambda p, e, idx: (e + off, p, 0, 0))
    ins = [pl.BlockSpec(memory_space=pl.ANY)] * len(parts)
    out_shape = [jax.ShapeDtypeStruct((local, peers, block, hidden), bf16)]
    if scaled:
        ins += [spec(1, first), spec(hidden, first)]
        out_shape.append(jax.ShapeDtypeStruct((local, peers, block, LANES), f32))
    out = pl.pallas_call(
        functools.partial(unpack_kernel, ranges=ranges, scaled=scaled, empty=empty, block=block),
        grid_spec=pltpu.PrefetchScalarGridSpec(
            num_scalar_prefetch=1,
            grid=(peers, local),
            in_specs=ins,
            out_specs=[spec(s.shape[-1]) for s in out_shape],
            scratch_shapes=[
                pltpu.VMEM((2, empty + 8, sub, LANES), bf16),
                pltpu.VMEM((block * (sub + 1), LANES), f32),
                pltpu.SemaphoreType.DMA((2, len(parts))),
            ],
        ),
        out_shape=out_shape,
        compiler_params=pltpu.CompilerParams(vmem_limit_bytes=32 * MIB),
        cost_estimate=cost(3_500_000_000 * local, 8_000_000 * local),
    )(idx.reshape(-1), *parts, *((norm, y) if scaled else ()))
    return out if scaled else out[0]


def pack_kernel(idx_ref, *refs, ranges, rows, count):
    ins, outs, acc_ref = refs[:count], refs[count:-1], refs[-1]
    base = pl.program_id(0) * rows
    sub = outs[0].shape[2]
    pitch = sub + 1
    at = 0
    for ref in ins:
        for e in range(ref.shape[0]):
            block = ref.shape[2]
            for j in range(sub):
                acc_ref[pl.ds(at * pitch + j, block, stride=pitch), :] = ref[e, 0, :, j * LANES:(j + 1) * LANES].astype(f32)
            at += block
    for (low, high), out_ref in zip(ranges, outs):
        def store(t, row, out_ref=out_ref):
            out_ref[0, t] = row.astype(bf16)

        move_rows(idx_ref, base + low, high - low, lambda k: acc_ref[pl.ds(k * pitch, sub), :], store)


def pack_rows(idx, grads, ranges):
    peers, rows = idx.shape
    block, hidden = grads[0].shape[2:]
    sub = hidden // LANES
    total = sum(g.shape[0] for g in grads) * block
    return pl.pallas_call(
        functools.partial(pack_kernel, ranges=ranges, rows=rows, count=len(grads)),
        grid_spec=pltpu.PrefetchScalarGridSpec(
            num_scalar_prefetch=1,
            grid=(peers,),
            in_specs=[pl.BlockSpec((g.shape[0], 1, block, hidden), lambda p, idx: (0, p, 0, 0)) for g in grads],
            out_specs=[pl.BlockSpec((1, high - low, sub, LANES), lambda p, idx: (p, 0, 0, 0)) for low, high in ranges],
            scratch_shapes=[pltpu.VMEM((total * (sub + 1), LANES), f32)],
        ),
        out_shape=[jax.ShapeDtypeStruct((peers, high - low, sub, LANES), bf16) for low, high in ranges],
        compiler_params=pltpu.CompilerParams(vmem_limit_bytes=40 * MIB),
        cost_estimate=cost(15_000_000_000, 35_000_000),
    )(idx.reshape(-1), *grads)


def combine_kernel(slot_ref, *refs, ranges, rows):
    count = len(ranges)
    parts, (r_ref, gl_ref, wg_ref, out_ref, held, acc_ref, sem) = refs[:count], refs[count:]
    block = out_ref.shape[0]
    tokens = slot_ref.shape[0] // 2
    base = pl.program_id(0) * block

    sub = held.shape[1]
    pitch = sub + 1
    peers = parts[0].shape[0]

    @pl.when(pl.program_id(0) == 0)
    def _():
        copies = [pltpu.make_async_copy(part.at[p], held.at[pl.ds(p * rows + low, high - low)], sem.at[k, p])
                  for k, (part, (low, high)) in enumerate(zip(parts, ranges)) for p in range(peers)]
        for copy in copies:
            copy.start()
        held[peers * rows:] = jnp.zeros((held.shape[0] - peers * rows,) + held.shape[1:], bf16)
        for copy in copies:
            copy.wait()

    def step(i, _):
        ones = [slot_ref[base + i * 8 + u] for u in range(8)]
        twos = [slot_ref[base + tokens + i * 8 + u] for u in range(8)]
        sums = [held[one].astype(f32) + held[two].astype(f32) for one, two in zip(ones, twos)]
        for u, row in enumerate(sums):
            acc_ref[pl.ds((i * 8 + u) * pitch, sub), :] = row
        return 0

    lax.fori_loop(0, block // 8, step, 0)
    router = lax.dot_general(gl_ref[...], wg_ref[...], (((1,), (1,)), ((), ())), preferred_element_type=f32)
    for j in range(sub):
        cols = slice(j * LANES, (j + 1) * LANES)
        out_ref[:, cols] = (r_ref[:, cols].astype(f32) + acc_ref[pl.ds(j, block, stride=pitch), :] + router[:, cols]).astype(bf16)


def combine_rows(slots_of, parts, ranges, r_rows, grad_logits, w_gate):
    tokens, hidden = r_rows.shape
    experts = w_gate.shape[1]
    peers, sub = parts[0].shape[0], parts[0].shape[2]
    rows = ranges[-1][1]
    block = 256
    return pl.pallas_call(
        functools.partial(combine_kernel, ranges=ranges, rows=rows),
        grid_spec=pltpu.PrefetchScalarGridSpec(
            num_scalar_prefetch=1,
            grid=(tokens // block,),
            in_specs=[pl.BlockSpec(memory_space=pl.ANY)] * len(parts) + [
                pl.BlockSpec((block, hidden), lambda b, s: (b, 0)),
                pl.BlockSpec((block, experts), lambda b, s: (b, 0)),
                pl.BlockSpec((hidden, experts), lambda b, s: (0, 0)),
            ],
            out_specs=pl.BlockSpec((block, hidden), lambda b, s: (b, 0)),
            scratch_shapes=[
                pltpu.VMEM((peers * rows + 8, sub, LANES), bf16),
                pltpu.VMEM((block * (sub + 1), LANES), f32),
                pltpu.SemaphoreType.DMA((len(parts), peers)),
            ],
        ),
        out_shape=jax.ShapeDtypeStruct(r_rows.shape, bf16),
        compiler_params=pltpu.CompilerParams(vmem_limit_bytes=52 * MIB),
        cost_estimate=cost(50_000_000_000, 80_000_000),
    )(slots_of.reshape(-1), *parts, r_rows, grad_logits, w_gate)


def solution(mesh):
    ep_size = mesh.shape['ep']

    def layer_body(x_loc, r_loc, w_gate, w_in_loc, w_out_loc, first_ids, second_ids, keep_ids):
        groups, seq_len, hidden = x_loc.shape
        experts = w_gate.shape[1]
        local_experts = experts // ep_size
        half = local_experts // 2
        cap_rows = 2 * seq_len // experts
        block = groups * cap_rows
        rows = local_experts * block
        mid = rows // 2
        base = rows * BASE_OUT // 32
        over = rows * (32 - BASE_BACK) // 32
        sub = hidden // LANES
        tokens_loc = groups * seq_len
        tokens_all = tokens_loc * ep_size
        numel = tokens_all * hidden
        exchange = lambda v: lax.all_to_all(v, 'ep', 0, 0, tiled=True)

        expert_ids = jnp.arange(experts, dtype=jnp.int32)
        first_hot = (first_ids[..., None] == expert_ids).astype(bf16)
        second_hot = (second_ids[..., None] == expert_ids).astype(bf16)
        second_kept = second_hot * keep_ids.astype(bf16)[..., None]
        seq_ids = jnp.arange(seq_len, dtype=jnp.int32)
        earlier = (seq_ids[:, None] > seq_ids[None, :]).astype(bf16)
        before_first = jnp.einsum('st,gte->gse', earlier, first_hot, preferred_element_type=f32)
        before_second = jnp.einsum('st,gte->gse', earlier, second_kept, preferred_element_type=f32)
        first_count = jnp.sum(first_hot, axis=1, dtype=f32)
        occupied = jnp.minimum(first_count + jnp.sum(second_kept, axis=1, dtype=f32), cap_rows)
        segments = lambda v: jnp.moveaxis(v.reshape(groups, ep_size, local_experts), 0, 2).reshape(ep_size, local_experts * groups)
        unsegment = lambda v: jnp.moveaxis(v.reshape(ep_size, local_experts, groups), 2, 0).reshape(groups, experts)
        peers = jnp.arange(ep_size, dtype=f32)[:, None]
        look = lambda hot, table: jnp.sum(table * hot, axis=-1)
        held = segments(occupied)
        back_at = unsegment(peers * rows + rows - jnp.sum(held, axis=1, keepdims=True) + jnp.cumsum(held, axis=1) - held)[:, None, :]
        pos_first = look(first_hot, before_first)
        pos_second = look(second_hot, before_second + first_count[:, None, :])
        ok_first = pos_first < cap_rows
        ok_second = (keep_ids > 0) & (pos_second < cap_rows)
        slots_of = jnp.stack([
            jnp.where(ok_first, (look(first_hot, back_at) + pos_first).astype(jnp.int32), ep_size * rows),
            jnp.where(ok_second, (look(second_hot, back_at) + pos_second).astype(jnp.int32), ep_size * rows),
        ])
        pos_first, pos_second = pos_first.astype(jnp.int32), pos_second.astype(jnp.int32)

        both = ok_first & ok_second & (first_ids // local_experts == second_ids // local_experts)
        goes_first = ok_first & ~(both & (second_ids < first_ids))
        goes_second = ok_second & ~(both & (first_ids < second_ids))
        first_goes = first_hot * goes_first.astype(bf16)[..., None]
        second_goes = second_hot * goes_second.astype(bf16)[..., None]
        ahead_first = jnp.einsum('st,gte->gse', earlier, first_goes, preferred_element_type=f32)
        ahead_second = jnp.einsum('st,gte->gse', earlier, second_goes, preferred_element_type=f32)
        first_gone = jnp.sum(first_goes, axis=1, dtype=f32)
        sent = segments(first_gone + jnp.sum(second_goes, axis=1, dtype=f32))
        out_at = unsegment(jnp.cumsum(sent, axis=1) - sent)[:, None, :]
        out_first = look(first_hot, ahead_first + out_at).astype(jnp.int32)
        out_second = look(second_hot, ahead_second + out_at + first_gone[:, None, :]).astype(jnp.int32)
        there = jnp.stack([
            jnp.where(goes_first, first_ids // local_experts * rows + out_first, -1),
            jnp.where(goes_second, second_ids // local_experts * rows + out_second, -1),
        ]).reshape(-1)
        read_first = jnp.where(goes_first, out_first, out_second) + 1
        read_second = jnp.where(goes_second, out_second, out_first) + 1
        numbers = jnp.arange(2 * tokens_loc, dtype=jnp.int32) % tokens_loc + 1
        outer = ((there // 64)[:, None] == jnp.arange(ep_size * rows // 64, dtype=jnp.int32)).astype(bf16)
        inner = ((there % 64)[:, None] == jnp.arange(64, dtype=jnp.int32)) & (there >= 0)[:, None]
        digits = jnp.concatenate([jnp.where(inner, v.astype(bf16)[:, None], 0) for v in (numbers // 64, numbers % 64)], axis=-1)
        table = jnp.einsum('so,si->oi', outer, digits, preferred_element_type=f32)
        send_idx = jnp.maximum((table[:, :64] * 64 + table[:, 64:]).astype(jnp.int32) - 1, 0).reshape(ep_size, rows)

        x_tiles = x_loc.reshape(tokens_loc, sub, LANES)
        r_tiles = r_loc.reshape(tokens_loc, sub, LANES)
        more = base + MORE
        x_ranges = ((0, base), (base, more), (more, rows))
        r_ranges = ((0, mid), (mid, base), (base, more), (more, rows))
        g_ranges = ((0, over - MORE), (over - MORE, over), (over, mid), (mid, rows))
        x_from = ((0, base, 0), (base, more, 0), (more, rows, 0))
        r_from = ((0, mid, 0), (mid, base, 0), (base, more, MORE), (more, rows, rows - more))
        x_send, x_more, x_rest = gather_rows(send_idx, x_tiles, x_ranges)

        tie = lambda *values: lax.optimization_barrier(values)
        x_recv = exchange(x_send)
        x_here, r_here, r_tiles, _ = tie(x_loc, r_loc, r_tiles, x_send)
        r_send_0, r_send_1, r_more, r_rest = gather_rows(send_idx, r_tiles, r_ranges)

        logits = jnp.einsum('gsh,he->gse', x_here, w_gate, preferred_element_type=f32)
        router_prob = jax.nn.softmax(logits, axis=-1)
        gate_first = jnp.sum(router_prob * first_hot, axis=-1)
        gate_second = jnp.sum(router_prob * second_hot, axis=-1)
        gate_sum = gate_first + gate_second
        norm_first = (gate_first / gate_sum).astype(bf16)
        norm_second = (gate_second / gate_sum).astype(bf16)
        slots = jnp.arange(cap_rows, dtype=jnp.int32)
        at_first = ((pos_first[..., None] == slots) & ok_first[..., None]).astype(bf16)
        at_second = ((pos_second[..., None] == slots) & ok_second[..., None]).astype(bf16)
        hots = jnp.concatenate([first_hot, second_hot], axis=1)
        digits_at = lambda at, *vs: jnp.concatenate([at * v.astype(bf16)[..., None] for v in vs], axis=-1)
        norm_at = jnp.concatenate([
            digits_at(at_first, norm_first, read_first // 64, read_first % 64),
            digits_at(at_second, norm_second, read_second // 64, read_second % 64),
        ], axis=1)
        slot_norm, slot_high, slot_low = jnp.split(jnp.einsum('gse,gsk->egk', hots, norm_at, preferred_element_type=f32), 3, axis=-1)
        slot_read = slot_high * 64 + slot_low
        dot_xr = jnp.sum(x_here.astype(f32) * r_here.astype(f32))
        to_rows = lambda v: jnp.moveaxis(v, 0, 1)[..., None]
        degree = lambda v, top: jnp.sum(jnp.max(jnp.sum(v, axis=1)) > jnp.array([top, top + MORE], f32)).astype(f32)
        levels = jnp.broadcast_to(jnp.stack([degree(sent, base), degree(held, rows - over)]), (experts, groups, 2))
        tally = jnp.moveaxis(first_count.reshape(groups, local_experts, ep_size), 0, 1)
        tally = jnp.tile(tally, (ep_size, 1, 1))
        sheet = jnp.concatenate([slot_norm, slot_read, levels, to_rows(occupied), tally], axis=-1)
        sheet, x_recv = tie(sheet, x_recv)
        sheet = lax.all_to_all(sheet, 'ep', 0, 1, tiled=True).reshape(local_experts, ep_size, groups, -1)
        expert_norm = sheet[..., :cap_rows].reshape(local_experts, ep_size, block)
        sheet_read, sheet = sheet[..., cap_rows:2 * cap_rows], sheet[..., 2 * cap_rows:]
        level_out, level_back = jnp.max(sheet[0, :, 0, :2], axis=0).astype(jnp.int32)
        mine = jnp.moveaxis(sheet[..., 2], 0, 1).reshape(ep_size, local_experts * groups)
        frac_first = jnp.sum(sheet[..., 3:], axis=(1, 2)).reshape(experts) / tokens_all
        mine_ends = jnp.cumsum(mine, axis=1)
        recv_idx = jnp.where(sheet_read > 0, sheet_read - 1, float(rows)).astype(jnp.int32)
        recv_idx = jnp.moveaxis(recv_idx.reshape(local_experts, ep_size, block), 0, 1)
        packed = jnp.arange(rows, dtype=f32) - (rows - mine_ends[:, -1:])
        passed = (mine_ends[:, None, :] <= packed[..., None]).astype(f32)
        back_row = jnp.sum(passed, axis=-1) * cap_rows + packed - jnp.sum(passed * mine[:, None, :], axis=-1)
        back_idx = jnp.where(packed >= 0, back_row, 0.0).astype(jnp.int32)

        def exchange_over(level, few, rest):
            return lax.switch(level, (lambda u, v: (u, v), lambda u, v: (exchange(u), v), lambda u, v: (exchange(u), exchange(v))), few, rest)

        xr_more, xr_rest = jnp.concatenate([x_more, r_more], axis=1), jnp.concatenate([x_rest, r_rest], axis=1)
        xr_more, xr_rest, expert_norm = tie(xr_more, xr_rest, expert_norm)
        xr_more, xr_rest = exchange_over(level_out, xr_more, xr_rest)
        r_send_0, xr_more, xr_rest, dot_xr = tie(r_send_0, xr_more, xr_rest, dot_xr)
        r_recv_0 = exchange(r_send_0)
        expert_x = unpack_rows(recv_idx, [x_recv, xr_more, xr_rest], x_from, rows).reshape(local_experts, -1, hidden)
        pre_act = jnp.einsum('ech,ehf->ecf', expert_x, w_in_loc, preferred_element_type=f32)
        act_bf = gelu_bf16(pre_act)
        expert_y = jnp.einsum('ecf,efh->ech', act_bf, w_out_loc, preferred_element_type=f32).astype(bf16)

        r_send_1, expert_y, r_recv_0 = tie(r_send_1, expert_y, r_recv_0)
        r_recv_1 = exchange(r_send_1)

        def expert_bwd(parts, ranges, which):
            chunk = slice(which * half, (which + 1) * half)
            grad_y, dots = unpack_rows(recv_idx[:, chunk], parts, ranges, rows, expert_norm[..., None], expert_y.reshape(local_experts, ep_size, block, hidden), which * half)
            slot_dot = jnp.sum(dots, axis=-1)
            grad_y = grad_y.reshape(half, -1, hidden)
            grad_act = jnp.einsum('ech,efh->ecf', grad_y, w_out_loc[chunk], preferred_element_type=f32).astype(bf16)
            grad_pre = jax.vjp(gelu_bf16, pre_act[chunk])[1](grad_act)[0].astype(bf16)
            grad_slots = jnp.einsum('ecf,ehf->ech', grad_pre, w_in_loc[chunk], preferred_element_type=f32).astype(bf16)
            return grad_y, grad_pre, slot_dot, grad_slots.reshape(half, ep_size, block, hidden)

        grad_y_0, grad_pre_0, slot_dot_0, grad_slots_0 = expert_bwd([r_recv_0], r_from[:1], 0)
        g_rest, g_more, g_send_0 = pack_rows(back_idx, [grad_slots_0], g_ranges[:3])
        g_more, g_rest, r_recv_1 = tie(g_more, g_rest, r_recv_1)
        g_more, g_rest = exchange_over(level_back, g_more, g_rest)
        g_send_0, g_more, g_rest, r_recv_1 = tie(g_send_0, g_more, g_rest, r_recv_1)
        g_recv_0 = exchange(g_send_0)
        grad_y_1, grad_pre_1, slot_dot_1, grad_slots_1 = expert_bwd([r_recv_0, r_recv_1, xr_more, xr_rest], r_from, 1)
        g_send_1, = pack_rows(back_idx, [grad_slots_0, grad_slots_1], g_ranges[3:])
        slot_dot = jnp.concatenate([slot_dot_0, slot_dot_1], axis=0)
        slot_dot, g_send_1, g_recv_0 = tie(slot_dot, g_send_1, g_recv_0)
        home_dot = lax.all_to_all(slot_dot.reshape(local_experts, ep_size * groups, cap_rows), 'ep', 1, 0, tiled=True)
        g_send_1, home_dot = tie(g_send_1, home_dot)
        g_recv_1 = exchange(g_send_1)

        grad_y = jnp.concatenate([grad_y_0, grad_y_1], axis=0)
        grad_pre = jnp.concatenate([grad_pre_0, grad_pre_1], axis=0)
        grad_w_out = jnp.einsum('ecf,ech->efh', act_bf, grad_y, preferred_element_type=f32).astype(bf16)
        grad_w_in = jnp.einsum('ech,ecf->ehf', expert_x, grad_pre, preferred_element_type=f32).astype(bf16)

        picked = lambda hot, at: jnp.sum(jnp.einsum('gse,egk->gsk', hot.astype(f32), home_dot, precision=lax.Precision.HIGHEST, preferred_element_type=f32) * at, axis=-1)
        grad_norm_first = picked(first_hot, at_first).astype(bf16).astype(f32)
        grad_norm_second = picked(second_hot, at_second).astype(bf16).astype(f32)
        gate_sq = gate_sum * gate_sum
        grad_gate_first = (grad_norm_first - grad_norm_second) * gate_second / gate_sq
        grad_gate_second = (grad_norm_second - grad_norm_first) * gate_first / gate_sq
        grad_prob = grad_gate_first[..., None] * first_hot + grad_gate_second[..., None] * second_hot + (ALPHA * hidden * experts) * frac_first
        grad_logits = router_prob * (grad_prob - jnp.sum(router_prob * grad_prob, axis=-1, keepdims=True))
        grad_logits_bf = grad_logits.astype(bf16)
        grad_gate_w = jnp.einsum('gsh,gse->he', x_loc, grad_logits_bf, preferred_element_type=f32)
        dot_sum = dot_xr + jnp.sum(slot_dot * expert_norm)
        stats = jnp.stack([jnp.sum(router_prob, axis=(0, 1)), jnp.broadcast_to(dot_sum, (experts,))])
        summed = lax.psum(jnp.concatenate([grad_gate_w, stats], axis=0), 'ep')
        grad_gate_w, prob_sum, dot_sum = summed[:hidden], summed[hidden], summed[hidden + 1, 0]
        loss_value = dot_sum / numel + ALPHA * experts * jnp.sum(frac_first * prob_sum / tokens_all)

        grad_x = combine_rows(slots_of, [g_rest, g_more, g_recv_0, g_recv_1], g_ranges, r_loc.reshape(-1, hidden), grad_logits_bf.reshape(-1, experts), w_gate)
        return loss_value, grad_x.reshape(x_loc.shape), grad_w_in, grad_w_out, grad_gate_w

    row_spec = P('ep', None, None)
    id_spec = P('ep', None)
    return jax.shard_map(layer_body, mesh=mesh, in_specs=(row_spec, row_spec, P(None, None), row_spec, row_spec, id_spec, id_spec, id_spec), out_specs=(P(), row_spec, row_spec, row_spec, P(None, None)), check_vma=False)
```

```python
import functools

import jax
import jax.numpy as jnp
from jax import lax
from jax.experimental import pallas as pl
from jax.experimental.pallas import tpu as pltpu
from jax.sharding import PartitionSpec as P


ALPHA = 0.01
LANES = 128
MIB = 1024 * 1024
BATCH = 16
BASE_OUT, BASE_BACK = 26, 27
STEPS = (32, 32)
bf16, f32 = jnp.bfloat16, jnp.float32


def gelu_bf16(pre_act):
    return jax.nn.gelu(pre_act, approximate=True).astype(bf16)


def cost(flops, moved):
    return pl.CostEstimate(flops=flops, bytes_accessed=moved, transcendentals=0)


def move_rows(idx_ref, base, count, load, store):
    def step(i, _):
        ids = [idx_ref[base + i * BATCH + u] for u in range(BATCH)]
        for u, row in enumerate([load(k) for k in ids]):
            store(i * BATCH + u, row)
        return 0

    lax.fori_loop(0, count // BATCH, step, 0)


def gather_kernel(idx_ref, tiles_ref, *outs, ranges, rows):
    base = pl.program_id(0) * rows
    for (low, high), out_ref in zip(ranges, outs):
        def store(t, row, out_ref=out_ref):
            out_ref[0, t] = row

        move_rows(idx_ref, base + low, high - low, lambda k: tiles_ref[k], store)


def gather_rows(idx, tiles, ranges):
    peers, rows = idx.shape
    count, sub, _ = tiles.shape
    return pl.pallas_call(
        functools.partial(gather_kernel, ranges=ranges, rows=rows),
        grid_spec=pltpu.PrefetchScalarGridSpec(
            num_scalar_prefetch=1,
            grid=(peers,),
            in_specs=[pl.BlockSpec((count, sub, LANES), lambda p, idx: (0, 0, 0))],
            out_specs=[pl.BlockSpec((1, high - low, sub, LANES), lambda p, idx: (p, 0, 0, 0)) for low, high in ranges],
        ),
        out_shape=[jax.ShapeDtypeStruct((peers, high - low, sub, LANES), tiles.dtype) for low, high in ranges],
        compiler_params=pltpu.CompilerParams(vmem_limit_bytes=52 * MIB),
        cost_estimate=cost(30_000_000_000, 60_000_000),
    )(idx.reshape(-1), tiles)


def unpack_kernel(idx_ref, *refs, ranges, scaled, empty, block):
    count = len(ranges)
    parts, refs = refs[:count], refs[count:]
    if scaled:
        norm_ref, y_ref, out_ref, dot_ref, packed, acc_ref, sem = refs
    else:
        out_ref, packed, acc_ref, sem = refs
    peer, local = pl.program_id(0), pl.program_id(1)
    slot = lax.rem(peer, 2)

    def copies(p, s):
        return [pltpu.make_async_copy(part.at[p, pl.ds(at, high - low)], packed.at[s, pl.ds(low, high - low)], sem.at[s, k])
                for k, (part, (low, high, at)) in enumerate(zip(parts, ranges))]

    @pl.when((peer == 0) & (local == 0))
    def _():
        blank = jnp.zeros((2, packed.shape[1] - empty) + packed.shape[2:], bf16)
        packed[:, empty:] = blank
        for copy in copies(0, 0):
            copy.start()

    @pl.when(local == 0)
    def _():
        @pl.when(peer + 1 < pl.num_programs(0))
        def _():
            for copy in copies(peer + 1, 1 - slot):
                copy.start()

        for copy in copies(peer, slot):
            copy.wait()

    base = (peer * pl.num_programs(1) + local) * block
    sub = packed.shape[2]
    pitch = sub + 1

    def store(t, row):
        acc_ref[pl.ds(t * pitch, sub), :] = row.astype(f32)

    move_rows(idx_ref, base, block, lambda k: packed[slot, k], store)
    total = None
    for j in range(sub):
        cols = slice(j * LANES, (j + 1) * LANES)
        tile = acc_ref[pl.ds(j, block, stride=pitch), :]
        if scaled:
            out_ref[0, 0, :, cols] = (norm_ref[0, 0] * tile).astype(bf16)
            product = y_ref[0, 0, :, cols].astype(f32) * tile
            total = product if total is None else total + product
        else:
            out_ref[0, 0, :, cols] = tile.astype(bf16)
    if scaled:
        dot_ref[0, 0] = total


def unpack_rows(idx, parts, ranges, empty, norm=None, y=None, first=0):
    peers, local, block = idx.shape
    sub = parts[0].shape[2]
    hidden = sub * LANES
    scaled = norm is not None
    spec = lambda width, off=0: pl.BlockSpec((1, 1, block, width), lambda p, e, idx: (e + off, p, 0, 0))
    ins = [pl.BlockSpec(memory_space=pl.ANY)] * len(parts)
    out_shape = [jax.ShapeDtypeStruct((local, peers, block, hidden), bf16)]
    if scaled:
        ins += [spec(1, first), spec(hidden, first)]
        out_shape.append(jax.ShapeDtypeStruct((local, peers, block, LANES), f32))
    out = pl.pallas_call(
        functools.partial(unpack_kernel, ranges=ranges, scaled=scaled, empty=empty, block=block),
        grid_spec=pltpu.PrefetchScalarGridSpec(
            num_scalar_prefetch=1,
            grid=(peers, local),
            in_specs=ins,
            out_specs=[spec(s.shape[-1]) for s in out_shape],
            scratch_shapes=[
                pltpu.VMEM((2, empty + 8, sub, LANES), bf16),
                pltpu.VMEM((block * (sub + 1), LANES), f32),
                pltpu.SemaphoreType.DMA((2, len(parts))),
            ],
        ),
        out_shape=out_shape,
        compiler_params=pltpu.CompilerParams(vmem_limit_bytes=32 * MIB),
        cost_estimate=cost(3_500_000_000 * local, 8_000_000 * local),
    )(idx.reshape(-1), *parts, *((norm, y) if scaled else ()))
    return out if scaled else out[0]


def pack_kernel(idx_ref, *refs, ranges, rows, count):
    ins, outs, acc_ref = refs[:count], refs[count:-1], refs[-1]
    base = pl.program_id(0) * rows
    sub = outs[0].shape[2]
    pitch = sub + 1
    at = 0
    for ref in ins:
        for e in range(ref.shape[0]):
            block = ref.shape[2]
            for j in range(sub):
                acc_ref[pl.ds(at * pitch + j, block, stride=pitch), :] = ref[e, 0, :, j * LANES:(j + 1) * LANES].astype(f32)
            at += block
    for (low, high), out_ref in zip(ranges, outs):
        def store(t, row, out_ref=out_ref):
            out_ref[0, t] = row.astype(bf16)

        move_rows(idx_ref, base + low, high - low, lambda k: acc_ref[pl.ds(k * pitch, sub), :], store)


def pack_rows(idx, grads, ranges):
    peers, rows = idx.shape
    block, hidden = grads[0].shape[2:]
    sub = hidden // LANES
    total = sum(g.shape[0] for g in grads) * block
    return pl.pallas_call(
        functools.partial(pack_kernel, ranges=ranges, rows=rows, count=len(grads)),
        grid_spec=pltpu.PrefetchScalarGridSpec(
            num_scalar_prefetch=1,
            grid=(peers,),
            in_specs=[pl.BlockSpec((g.shape[0], 1, block, hidden), lambda p, idx: (0, p, 0, 0)) for g in grads],
            out_specs=[pl.BlockSpec((1, high - low, sub, LANES), lambda p, idx: (p, 0, 0, 0)) for low, high in ranges],
            scratch_shapes=[pltpu.VMEM((total * (sub + 1), LANES), f32)],
        ),
        out_shape=[jax.ShapeDtypeStruct((peers, high - low, sub, LANES), bf16) for low, high in ranges],
        compiler_params=pltpu.CompilerParams(vmem_limit_bytes=40 * MIB),
        cost_estimate=cost(15_000_000_000, 35_000_000),
    )(idx.reshape(-1), *grads)


def combine_kernel(slot_ref, *refs, ranges, rows):
    count = len(ranges)
    parts, (r_ref, gl_ref, wg_ref, out_ref, held, acc_ref, sem) = refs[:count], refs[count:]
    block = out_ref.shape[0]
    tokens = slot_ref.shape[0] // 2
    base = pl.program_id(0) * block

    sub = held.shape[1]
    pitch = sub + 1
    peers = parts[0].shape[0]

    @pl.when(pl.program_id(0) == 0)
    def _():
        copies = [pltpu.make_async_copy(part.at[p], held.at[pl.ds(p * rows + low, high - low)], sem.at[k, p])
                  for k, (part, (low, high)) in enumerate(zip(parts, ranges)) for p in range(peers)]
        for copy in copies:
            copy.start()
        held[peers * rows:] = jnp.zeros((held.shape[0] - peers * rows,) + held.shape[1:], bf16)
        for copy in copies:
            copy.wait()

    def step(i, _):
        ones = [slot_ref[base + i * 8 + u] for u in range(8)]
        twos = [slot_ref[base + tokens + i * 8 + u] for u in range(8)]
        sums = [held[one].astype(f32) + held[two].astype(f32) for one, two in zip(ones, twos)]
        for u, row in enumerate(sums):
            acc_ref[pl.ds((i * 8 + u) * pitch, sub), :] = row
        return 0

    lax.fori_loop(0, block // 8, step, 0)
    router = lax.dot_general(gl_ref[...], wg_ref[...], (((1,), (1,)), ((), ())), preferred_element_type=f32)
    for j in range(sub):
        cols = slice(j * LANES, (j + 1) * LANES)
        out_ref[:, cols] = (r_ref[:, cols].astype(f32) + acc_ref[pl.ds(j, block, stride=pitch), :] + router[:, cols]).astype(bf16)


def combine_rows(slots_of, parts, ranges, r_rows, grad_logits, w_gate):
    tokens, hidden = r_rows.shape
    experts = w_gate.shape[1]
    peers, sub = parts[0].shape[0], parts[0].shape[2]
    rows = ranges[-1][1]
    block = 256
    return pl.pallas_call(
        functools.partial(combine_kernel, ranges=ranges, rows=rows),
        grid_spec=pltpu.PrefetchScalarGridSpec(
            num_scalar_prefetch=1,
            grid=(tokens // block,),
            in_specs=[pl.BlockSpec(memory_space=pl.ANY)] * len(parts) + [
                pl.BlockSpec((block, hidden), lambda b, s: (b, 0)),
                pl.BlockSpec((block, experts), lambda b, s: (b, 0)),
                pl.BlockSpec((hidden, experts), lambda b, s: (0, 0)),
            ],
            out_specs=pl.BlockSpec((block, hidden), lambda b, s: (b, 0)),
            scratch_shapes=[
                pltpu.VMEM((peers * rows + 8, sub, LANES), bf16),
                pltpu.VMEM((block * (sub + 1), LANES), f32),
                pltpu.SemaphoreType.DMA((len(parts), peers)),
            ],
        ),
        out_shape=jax.ShapeDtypeStruct(r_rows.shape, bf16),
        compiler_params=pltpu.CompilerParams(vmem_limit_bytes=52 * MIB),
        cost_estimate=cost(50_000_000_000, 80_000_000),
    )(slots_of.reshape(-1), *parts, r_rows, grad_logits, w_gate)


def solution(mesh):
    ep_size = mesh.shape['ep']

    def layer_body(x_loc, r_loc, w_gate, w_in_loc, w_out_loc, first_ids, second_ids, keep_ids):
        groups, seq_len, hidden = x_loc.shape
        experts = w_gate.shape[1]
        local_experts = experts // ep_size
        half = local_experts // 2
        cap_rows = 2 * seq_len // experts
        block = groups * cap_rows
        rows = local_experts * block
        mid = rows // 2
        base = rows * BASE_OUT // 32
        over = rows * (32 - BASE_BACK) // 32
        sub = hidden // LANES
        tokens_loc = groups * seq_len
        tokens_all = tokens_loc * ep_size
        numel = tokens_all * hidden
        exchange = lambda v: lax.all_to_all(v, 'ep', 0, 0, tiled=True)

        expert_ids = jnp.arange(experts, dtype=jnp.int32)
        first_hot = (first_ids[..., None] == expert_ids).astype(bf16)
        second_hot = (second_ids[..., None] == expert_ids).astype(bf16)
        second_kept = second_hot * keep_ids.astype(bf16)[..., None]
        seq_ids = jnp.arange(seq_len, dtype=jnp.int32)
        earlier = (seq_ids[:, None] > seq_ids[None, :]).astype(bf16)
        before_first = jnp.einsum('st,gte->gse', earlier, first_hot, preferred_element_type=f32)
        before_second = jnp.einsum('st,gte->gse', earlier, second_kept, preferred_element_type=f32)
        first_count = jnp.sum(first_hot, axis=1, dtype=f32)
        occupied = jnp.minimum(first_count + jnp.sum(second_kept, axis=1, dtype=f32), cap_rows)
        segments = lambda v: jnp.moveaxis(v.reshape(groups, ep_size, local_experts), 0, 2).reshape(ep_size, local_experts * groups)
        unsegment = lambda v: jnp.moveaxis(v.reshape(ep_size, local_experts, groups), 2, 0).reshape(groups, experts)
        peers = jnp.arange(ep_size, dtype=f32)[:, None]
        look = lambda hot, table: jnp.sum(table * hot, axis=-1)
        held = segments(occupied)
        back_at = unsegment(peers * rows + rows - jnp.sum(held, axis=1, keepdims=True) + jnp.cumsum(held, axis=1) - held)[:, None, :]
        pos_first = look(first_hot, before_first)
        pos_second = look(second_hot, before_second + first_count[:, None, :])
        ok_first = pos_first < cap_rows
        ok_second = (keep_ids > 0) & (pos_second < cap_rows)
        slots_of = jnp.stack([
            jnp.where(ok_first, (look(first_hot, back_at) + pos_first).astype(jnp.int32), ep_size * rows),
            jnp.where(ok_second, (look(second_hot, back_at) + pos_second).astype(jnp.int32), ep_size * rows),
        ])
        pos_first, pos_second = pos_first.astype(jnp.int32), pos_second.astype(jnp.int32)

        both = ok_first & ok_second & (first_ids // local_experts == second_ids // local_experts)
        goes_first = ok_first & ~(both & (second_ids < first_ids))
        goes_second = ok_second & ~(both & (first_ids < second_ids))
        first_goes = first_hot * goes_first.astype(bf16)[..., None]
        second_goes = second_hot * goes_second.astype(bf16)[..., None]
        ahead_first = jnp.einsum('st,gte->gse', earlier, first_goes, preferred_element_type=f32)
        ahead_second = jnp.einsum('st,gte->gse', earlier, second_goes, preferred_element_type=f32)
        first_gone = jnp.sum(first_goes, axis=1, dtype=f32)
        sent = segments(first_gone + jnp.sum(second_goes, axis=1, dtype=f32))
        out_at = unsegment(jnp.cumsum(sent, axis=1) - sent)[:, None, :]
        out_first = look(first_hot, ahead_first + out_at).astype(jnp.int32)
        out_second = look(second_hot, ahead_second + out_at + first_gone[:, None, :]).astype(jnp.int32)
        there = jnp.stack([
            jnp.where(goes_first, first_ids // local_experts * rows + out_first, -1),
            jnp.where(goes_second, second_ids // local_experts * rows + out_second, -1),
        ]).reshape(-1)
        read_first = jnp.where(goes_first, out_first, out_second) + 1
        read_second = jnp.where(goes_second, out_second, out_first) + 1
        numbers = jnp.arange(2 * tokens_loc, dtype=jnp.int32) % tokens_loc + 1
        outer = ((there // 64)[:, None] == jnp.arange(ep_size * rows // 64, dtype=jnp.int32)).astype(bf16)
        inner = ((there % 64)[:, None] == jnp.arange(64, dtype=jnp.int32)) & (there >= 0)[:, None]
        digits = jnp.concatenate([jnp.where(inner, v.astype(bf16)[:, None], 0) for v in (numbers // 64, numbers % 64)], axis=-1)
        table = jnp.einsum('so,si->oi', outer, digits, preferred_element_type=f32)
        send_idx = jnp.maximum((table[:, :64] * 64 + table[:, 64:]).astype(jnp.int32) - 1, 0).reshape(ep_size, rows)

        x_tiles = x_loc.reshape(tokens_loc, sub, LANES)
        r_tiles = r_loc.reshape(tokens_loc, sub, LANES)
        extra = lambda start: [start + sum(STEPS[:k]) for k in range(len(STEPS) + 1)]
        spans = lambda edges: tuple(zip(edges[:-1], edges[1:]))
        out_over = spans(extra(base) + [rows])
        back_over = spans([0] + [rows - v for v in extra(rows - over)[::-1]])
        x_ranges = ((0, base), *out_over)
        r_ranges = ((0, mid), (mid, base), *out_over)
        g_ranges = (*back_over, (over, mid), (mid, rows))
        x_from = tuple((low, high, 0) for low, high in x_ranges)
        r_from = ((0, mid, 0), (mid, base, 0), *((low, high, high - low) for low, high in out_over))
        x_send, *x_over = gather_rows(send_idx, x_tiles, x_ranges)

        tie = lambda *values: lax.optimization_barrier(values)
        x_recv = exchange(x_send)
        x_here, r_here, r_tiles, _ = tie(x_loc, r_loc, r_tiles, x_send)
        r_send_0, r_send_1, *r_over = gather_rows(send_idx, r_tiles, r_ranges)

        logits = jnp.einsum('gsh,he->gse', x_here, w_gate, preferred_element_type=f32)
        router_prob = jax.nn.softmax(logits, axis=-1)
        gate_first = jnp.sum(router_prob * first_hot, axis=-1)
        gate_second = jnp.sum(router_prob * second_hot, axis=-1)
        gate_sum = gate_first + gate_second
        norm_first = (gate_first / gate_sum).astype(bf16)
        norm_second = (gate_second / gate_sum).astype(bf16)
        slots = jnp.arange(cap_rows, dtype=jnp.int32)
        at_first = ((pos_first[..., None] == slots) & ok_first[..., None]).astype(bf16)
        at_second = ((pos_second[..., None] == slots) & ok_second[..., None]).astype(bf16)
        hots = jnp.concatenate([first_hot, second_hot], axis=1)
        digits_at = lambda at, *vs: jnp.concatenate([at * v.astype(bf16)[..., None] for v in vs], axis=-1)
        norm_at = jnp.concatenate([
            digits_at(at_first, norm_first, read_first // 64, read_first % 64),
            digits_at(at_second, norm_second, read_second // 64, read_second % 64),
        ], axis=1)
        slot_norm, slot_high, slot_low = jnp.split(jnp.einsum('gse,gsk->egk', hots, norm_at, preferred_element_type=f32), 3, axis=-1)
        slot_read = slot_high * 64 + slot_low
        dot_xr = jnp.sum(x_here.astype(f32) * r_here.astype(f32))
        to_rows = lambda v: jnp.moveaxis(v, 0, 1)[..., None]
        degree = lambda v, top: jnp.sum(jnp.max(jnp.sum(v, axis=1)) > jnp.array(extra(top), f32)).astype(f32)
        levels = jnp.broadcast_to(jnp.stack([degree(sent, base), degree(held, rows - over)]), (experts, groups, 2))
        tally = jnp.moveaxis(first_count.reshape(groups, local_experts, ep_size), 0, 1)
        tally = jnp.tile(tally, (ep_size, 1, 1))
        sheet = jnp.concatenate([slot_norm, slot_read, levels, to_rows(occupied), tally], axis=-1)
        sheet, x_recv = tie(sheet, x_recv)
        sheet = lax.all_to_all(sheet, 'ep', 0, 1, tiled=True).reshape(local_experts, ep_size, groups, -1)
        expert_norm = sheet[..., :cap_rows].reshape(local_experts, ep_size, block)
        sheet_read, sheet = sheet[..., cap_rows:2 * cap_rows], sheet[..., 2 * cap_rows:]
        level_out, level_back = jnp.max(sheet[0, :, 0, :2], axis=0).astype(jnp.int32)
        mine = jnp.moveaxis(sheet[..., 2], 0, 1).reshape(ep_size, local_experts * groups)
        frac_first = jnp.sum(sheet[..., 3:], axis=(1, 2)).reshape(experts) / tokens_all
        mine_ends = jnp.cumsum(mine, axis=1)
        recv_idx = jnp.where(sheet_read > 0, sheet_read - 1, float(rows)).astype(jnp.int32)
        recv_idx = jnp.moveaxis(recv_idx.reshape(local_experts, ep_size, block), 0, 1)
        packed = jnp.arange(rows, dtype=f32) - (rows - mine_ends[:, -1:])
        passed = (mine_ends[:, None, :] <= packed[..., None]).astype(f32)
        back_row = jnp.sum(passed, axis=-1) * cap_rows + packed - jnp.sum(passed * mine[:, None, :], axis=-1)
        back_idx = jnp.where(packed >= 0, back_row, 0.0).astype(jnp.int32)

        def exchange_over(level, pieces):
            branch = lambda k: lambda *ps: tuple(exchange(p) if i < k else p for i, p in enumerate(ps))
            return lax.switch(level, [branch(k) for k in range(len(pieces) + 1)], *pieces)

        xr_over = [jnp.concatenate(pair, axis=1) for pair in zip(x_over, r_over)]
        *xr_over, expert_norm = tie(*xr_over, expert_norm)
        xr_over = exchange_over(level_out, xr_over)
        r_send_0, dot_xr, *xr_over = tie(r_send_0, dot_xr, *xr_over)
        r_recv_0 = exchange(r_send_0)
        expert_x = unpack_rows(recv_idx, [x_recv, *xr_over], x_from, rows).reshape(local_experts, -1, hidden)
        pre_act = jnp.einsum('ech,ehf->ecf', expert_x, w_in_loc, preferred_element_type=f32)
        act_bf = gelu_bf16(pre_act)
        expert_y = jnp.einsum('ecf,efh->ech', act_bf, w_out_loc, preferred_element_type=f32).astype(bf16)

        r_send_1, expert_y, r_recv_0 = tie(r_send_1, expert_y, r_recv_0)
        r_recv_1 = exchange(r_send_1)

        def expert_bwd(parts, ranges, which):
            chunk = slice(which * half, (which + 1) * half)
            grad_y, dots = unpack_rows(recv_idx[:, chunk], parts, ranges, rows, expert_norm[..., None], expert_y.reshape(local_experts, ep_size, block, hidden), which * half)
            slot_dot = jnp.sum(dots, axis=-1)
            grad_y = grad_y.reshape(half, -1, hidden)
            grad_act = jnp.einsum('ech,efh->ecf', grad_y, w_out_loc[chunk], preferred_element_type=f32).astype(bf16)
            grad_pre = jax.vjp(gelu_bf16, pre_act[chunk])[1](grad_act)[0].astype(bf16)
            grad_slots = jnp.einsum('ecf,ehf->ech', grad_pre, w_in_loc[chunk], preferred_element_type=f32).astype(bf16)
            return grad_y, grad_pre, slot_dot, grad_slots.reshape(half, ep_size, block, hidden)

        grad_y_0, grad_pre_0, slot_dot_0, grad_slots_0 = expert_bwd([r_recv_0], r_from[:1], 0)
        *g_over, g_send_0 = pack_rows(back_idx, [grad_slots_0], g_ranges[:-1])
        r_recv_1, *g_over = tie(r_recv_1, *g_over)
        g_over = exchange_over(level_back, g_over[::-1])[::-1]
        g_send_0, r_recv_1, *g_over = tie(g_send_0, r_recv_1, *g_over)
        g_recv_0 = exchange(g_send_0)
        grad_y_1, grad_pre_1, slot_dot_1, grad_slots_1 = expert_bwd([r_recv_0, r_recv_1, *xr_over], r_from, 1)
        g_send_1, = pack_rows(back_idx, [grad_slots_0, grad_slots_1], g_ranges[-1:])
        slot_dot = jnp.concatenate([slot_dot_0, slot_dot_1], axis=0)
        slot_dot, g_send_1, g_recv_0 = tie(slot_dot, g_send_1, g_recv_0)
        home_dot = lax.all_to_all(slot_dot.reshape(local_experts, ep_size * groups, cap_rows), 'ep', 1, 0, tiled=True)
        g_send_1, home_dot = tie(g_send_1, home_dot)
        g_recv_1 = exchange(g_send_1)

        grad_y = jnp.concatenate([grad_y_0, grad_y_1], axis=0)
        grad_pre = jnp.concatenate([grad_pre_0, grad_pre_1], axis=0)
        grad_w_out = jnp.einsum('ecf,ech->efh', act_bf, grad_y, preferred_element_type=f32).astype(bf16)
        grad_w_in = jnp.einsum('ech,ecf->ehf', expert_x, grad_pre, preferred_element_type=f32).astype(bf16)

        picked = lambda hot, at: jnp.sum(jnp.einsum('gse,egk->gsk', hot.astype(f32), home_dot, precision=lax.Precision.HIGHEST, preferred_element_type=f32) * at, axis=-1)
        grad_norm_first = picked(first_hot, at_first).astype(bf16).astype(f32)
        grad_norm_second = picked(second_hot, at_second).astype(bf16).astype(f32)
        gate_sq = gate_sum * gate_sum
        grad_gate_first = (grad_norm_first - grad_norm_second) * gate_second / gate_sq
        grad_gate_second = (grad_norm_second - grad_norm_first) * gate_first / gate_sq
        grad_prob = grad_gate_first[..., None] * first_hot + grad_gate_second[..., None] * second_hot + (ALPHA * hidden * experts) * frac_first
        grad_logits = router_prob * (grad_prob - jnp.sum(router_prob * grad_prob, axis=-1, keepdims=True))
        grad_logits_bf = grad_logits.astype(bf16)
        grad_gate_w = jnp.einsum('gsh,gse->he', x_loc, grad_logits_bf, preferred_element_type=f32)
        dot_sum = dot_xr + jnp.sum(slot_dot * expert_norm)
        stats = jnp.stack([jnp.sum(router_prob, axis=(0, 1)), jnp.broadcast_to(dot_sum, (experts,))])
        summed = lax.psum(jnp.concatenate([grad_gate_w, stats], axis=0), 'ep')
        grad_gate_w, prob_sum, dot_sum = summed[:hidden], summed[hidden], summed[hidden + 1, 0]
        loss_value = dot_sum / numel + ALPHA * experts * jnp.sum(frac_first * prob_sum / tokens_all)

        grad_x = combine_rows(slots_of, [*g_over, g_recv_0, g_recv_1], g_ranges, r_loc.reshape(-1, hidden), grad_logits_bf.reshape(-1, experts), w_gate)
        return loss_value, grad_x.reshape(x_loc.shape), grad_w_in, grad_w_out, grad_gate_w

    row_spec = P('ep', None, None)
    id_spec = P('ep', None)
    return jax.shard_map(layer_body, mesh=mesh, in_specs=(row_spec, row_spec, P(None, None), row_spec, row_spec, id_spec, id_spec, id_spec), out_specs=(P(), row_spec, row_spec, row_spec, P(None, None)), check_vma=False)
```
